32 devices in a mesh: dp: 4 (over z), tp: 8 (over y, x, core).
Axes of the slice: x: 2, y: 2, z: 4, core: 2. Of those that a mesh axis runs over, the one named last changes fastest.
Arguments:
- x_in: bfloat16 [3, 2, 48, 384, 1024], P(None, None, 'dp')
- u_pre: bfloat16 [3, 2, 48, 384, 4096], P(None, None, 'dp', None, 'tp')
- w_up: bfloat16 [3, 1024, 4096], P(None, None, 'tp')
- w_down: bfloat16 [3, 4096, 1024], P(None, 'tp')
- d_out: bfloat16 [2, 48, 384, 1024], P(None, 'dp')
- noise_up: float32 [3, 1024, 4096], P(None, 'dp', 'tp')
- noise_down: float32 [3, 4096, 1024], P(None, 'tp', 'dp')
- clip_norm: float32 [1], replicated
- noise_mult: float32 [1], replicated
Outputs:
- output 1: float32 [3, 1024, 4096], P(None, 'dp', 'tp')
- output 2: float32 [3, 4096, 1024], P(None, 'tp', 'dp')
- output 3: bfloat16 [2, 48, 384, 1024], P(None, 'dp')
All inputs are finite; a program needn't handle non-finite values.
Results may differ from the reference program's by a relative error of at most 0.0169951.
Values are sent between devices in bfloat16 or wider.
A program may use at most 1 GiB of HBM per device.

```python
import math
import jax
import jax.numpy as jnp
from jax import lax

LAYERS = 3
MICRO = 2
GLOBAL_BATCH = 48
SEQ_LEN = 384
D_MODEL = 1024
D_FF = 4096

EXAMPLES = MICRO * GLOBAL_BATCH


def setup_inputs(seed: int = 0) -> dict:
    base_key = jax.random.key(seed)
    key_list = jax.random.split(base_key, 10)
    act_shape = (LAYERS, MICRO, GLOBAL_BATCH, SEQ_LEN)
    x_in = jax.random.normal(key_list[0], act_shape + (D_MODEL,), jnp.float32).astype(jnp.bfloat16)
    u_pre = jax.random.normal(key_list[1], act_shape + (D_FF,), jnp.float32).astype(jnp.bfloat16)
    w_up = (jax.random.normal(key_list[2], (LAYERS, D_MODEL, D_FF), jnp.float32) * D_MODEL ** -0.5).astype(jnp.bfloat16)
    w_down = (jax.random.normal(key_list[3], (LAYERS, D_FF, D_MODEL), jnp.float32) * D_FF ** -0.5).astype(jnp.bfloat16)
    log_scale = jax.random.uniform(key_list[4], (MICRO, GLOBAL_BATCH, 1, 1), jnp.float32, math.log(0.5), math.log(16.0))
    d_out = (jax.random.normal(key_list[5], (MICRO, GLOBAL_BATCH, SEQ_LEN, D_MODEL), jnp.float32) * jnp.exp(log_scale)).astype(jnp.bfloat16)
    noise_up = jax.random.normal(key_list[6], (LAYERS, D_MODEL, D_FF), jnp.float32)
    noise_down = jax.random.normal(key_list[7], (LAYERS, D_FF, D_MODEL), jnp.float32)
    clip_norm = jax.random.uniform(key_list[8], (1,), jnp.float32, 0.6, 1.0) * math.sqrt(LAYERS * SEQ_LEN * D_MODEL * D_FF)
    noise_mult = jnp.exp(jax.random.uniform(key_list[9], (1,), jnp.float32, math.log(0.08), math.log(0.75))) * math.sqrt(EXAMPLES / (2.0 * LAYERS * D_MODEL * D_FF))
    return {"x_in": x_in, "u_pre": u_pre, "w_up": w_up, "w_down": w_down, "d_out": d_out, "noise_up": noise_up, "noise_down": noise_down, "clip_norm": clip_norm, "noise_mult": noise_mult}


def reference(x_in, u_pre, w_up, w_down, d_out, noise_up, noise_down, clip_norm, noise_mult):
    x_rows = x_in.reshape(LAYERS, EXAMPLES, SEQ_LEN, D_MODEL)
    u_rows = u_pre.reshape(LAYERS, EXAMPLES, SEQ_LEN, D_FF)
    top_cot = d_out.reshape(EXAMPLES, SEQ_LEN, D_MODEL)

    def layer_step(carry_in, layer_in):
        grad_cot, norm_vec = carry_in
        x_layer, u_layer, w_first, w_second = layer_in
        w_first_t = w_first.T
        w_second_t = w_second.T

        def one_example(example):
            x_ex, u_ex, cot_ex = example
            gelu_out, gelu_vjp = jax.vjp(jax.nn.gelu, u_ex.astype(jnp.float32))
            hidden = gelu_out.astype(jnp.bfloat16)
            d_act = jnp.dot(cot_ex, w_second_t, preferred_element_type=jnp.float32)
            d_hid = gelu_vjp(d_act)[0].astype(jnp.bfloat16)
            back_prop = jnp.dot(d_hid, w_first_t, preferred_element_type=jnp.float32)
            new_cot = (cot_ex.astype(jnp.float32) + back_prop).astype(jnp.bfloat16)
            gram_term = jnp.sum(jnp.dot(hidden, hidden.T, preferred_element_type=jnp.float32) * jnp.dot(cot_ex, cot_ex.T, preferred_element_type=jnp.float32))
            gram_term = gram_term + jnp.sum(jnp.dot(x_ex, x_ex.T, preferred_element_type=jnp.float32) * jnp.dot(d_hid, d_hid.T, preferred_element_type=jnp.float32))
            return new_cot, gram_term, hidden, d_hid

        new_cot, gram_add, hid_layer, dhid_layer = lax.map(one_example, (x_layer, u_layer, grad_cot))
        return (new_cot, norm_vec + gram_add), (hid_layer, dhid_layer, grad_cot)

    start_carry = (top_cot, jnp.zeros((EXAMPLES,), jnp.float32))
    (d_in, norm_vec), (hid_all, dhid_all, cot_all) = lax.scan(layer_step, start_carry, (x_rows, u_rows, w_up, w_down), reverse=True)
    clip_fac = jnp.minimum(1.0, clip_norm[0] / jnp.sqrt(norm_vec))
    scale_col = clip_fac[:, None, None]

    def weight_grads(layer_in):
        x_layer, hidden, d_hid, grad_cot = layer_in
        scaled_dh = (d_hid.astype(jnp.float32) * scale_col).astype(jnp.bfloat16)
        scaled_cot = (grad_cot.astype(jnp.float32) * scale_col).astype(jnp.bfloat16)
        up_grad = jnp.dot(x_layer.reshape(-1, D_MODEL).T, scaled_dh.reshape(-1, D_FF), preferred_element_type=jnp.float32)
        down_grad = jnp.dot(hidden.reshape(-1, D_FF).T, scaled_cot.reshape(-1, D_MODEL), preferred_element_type=jnp.float32)
        return up_grad, down_grad

    up_sum, down_sum = lax.map(weight_grads, (x_rows, hid_all, dhid_all, cot_all))
    noise_scale = noise_mult[0] * clip_norm[0]
    grad_up = (up_sum + noise_scale * noise_up) / EXAMPLES
    grad_down = (down_sum + noise_scale * noise_down) / EXAMPLES
    return grad_up, grad_down, d_in.reshape(MICRO, GLOBAL_BATCH, SEQ_LEN, D_MODEL)
```

```python
import functools
import math

import jax
import jax.numpy as jnp
from jax import lax
from jax.experimental import pallas as pl
from jax.experimental.pallas import tpu as pltpu
from jax.sharding import PartitionSpec as P

F32 = jnp.float32
BF16 = jnp.bfloat16
NT = (((1,), (1,)), ((), ()))
ANY = pl.BlockSpec(memory_space=pl.ANY)
VMEM = pl.BlockSpec(memory_space=pltpu.VMEM)
LAG = 2
U_GROUP = 4
COEF = math.sqrt(2.0 / math.pi)
CUBE = 0.044715


def place():
    t = lax.axis_index("tp")
    core = lax.rem(t, 2)
    px = lax.rem(lax.div(t, 2), 2)
    py = lax.div(t, 4)
    return core, px, py, t + 2 - 4 * px, t + 4 - 8 * py, t + 1 - 2 * core


def enter(peers):
    barrier = pltpu.get_barrier_semaphore()
    for peer in peers:
        pl.semaphore_signal(barrier, inc=1, device_id={"tp": peer}, device_id_type=pl.DeviceIdType.MESH)
    pl.semaphore_wait(barrier, len(peers))


def push(src, dst, send_sem, recv_sem, peer):
    return pltpu.make_async_remote_copy(src_ref=src, dst_ref=dst, send_sem=send_sem, recv_sem=recv_sem, device_id={"tp": peer}, device_id_type=pl.DeviceIdType.MESH)


class Exchange:
    def __init__(self, pos, part, cot, got1, got2, sems, n_examples, n_slots):
        self.core, self.px, self.py, self.nx, self.ny, self.partner = pos
        self.part, self.cot, self.got1, self.got2, self.sems = part, cot, got1, got2, sems
        self.n_examples, self.n_slots = n_examples, n_slots

    def copies(self, kind, j):
        px, py = self.px, self.py
        part = self.part.at[lax.rem(j, self.n_slots)]
        cot = self.cot.at[lax.rem(j, self.n_examples)]
        s = lax.rem(j, 4)
        send, recv = self.sems.at[0, kind], self.sems.at[1, kind]
        if kind == 0:
            pairs = ((part.at[pl.ds(2 * (1 - px), 2)], self.got1.at[s, 0], self.nx), (part.at[pl.ds(4 + 2 * (1 - py), 2)], self.got1.at[s, 1], self.ny))
        elif kind == 1:
            pairs = ((part.at[2 * px + 1 - py], self.got2.at[s, 0], self.ny), (part.at[4 + 2 * py + 1 - px], self.got2.at[s, 1], self.nx))
        elif kind == 2:
            own_a, own_b = cot.at[2 * px + py], cot.at[4 + 2 * py + px]
            pairs = ((own_a, own_a, self.ny), (own_b, own_b, self.nx))
        else:
            two_a, two_b = cot.at[pl.ds(2 * px, 2)], cot.at[pl.ds(4 + 2 * py, 2)]
            pairs = ((two_a, two_a, self.nx), (two_b, two_b, self.ny))
        return [push(src, dst, send.at[s, c], recv.at[s, c], peer) for c, (src, dst, peer) in enumerate(pairs)]

    def start(self, kind, j):
        for copy in self.copies(kind, j):
            copy.start()

    def wait(self, kind, j):
        for copy in self.copies(kind, j):
            copy.wait()

    def add_first(self, j):
        self.wait(0, j)
        slot, s = lax.rem(j, self.n_slots), lax.rem(j, 4)
        for c, first in enumerate((2 * self.px, 4 + 2 * self.py)):
            for i in range(2):
                mine = self.part[slot, first + i].astype(F32) + self.got1[s, c, i].astype(F32)
                self.part[slot, first + i] = mine.astype(BF16)
        self.start(1, j)

    def add_second(self, j):
        self.wait(1, j)
        slot, s, e = lax.rem(j, self.n_slots), lax.rem(j, 4), lax.rem(j, self.n_examples)
        for c, own in enumerate((2 * self.px + self.py, 4 + 2 * self.py + self.px)):
            back = self.part[slot, own].astype(F32) + self.got2[s, c].astype(F32)
            self.cot[e, own] = (self.cot[e, own].astype(F32) + back).astype(BF16)
        self.start(2, j)

    def forward(self, j):
        self.wait(2, j)
        self.start(3, j)


def run_stages(ex, k, count, save, saved):
    def at(lag, fn):
        j = k - lag * LAG

        @pl.when(jnp.logical_and(j >= 0, j < count))
        def _():
            fn(j)

    def finish(j):
        ex.wait(3, j)
        save(j)

    at(5, saved)
    at(4, finish)
    at(3, ex.forward)
    at(2, ex.add_second)
    at(1, ex.add_first)


def backward_kernel(u, x, w_up, w_down, d_out, dx_out, dh_out, part_out, norm_out, cot, w1, w2, u_own, u_far, x_buf, d_act, hid, dh, part, got1, got2, gram_a, gram_b, sems, w_sems, u_sems, cot_sems, load_sems, dh_sems, dx_sems, all_sems, part_sems):
    n_layers, _, n_ex, seq, d_ff = u.shape
    d_model = x.shape[-1]
    pieces = cot.shape[1:]
    groups = n_ex // U_GROUP
    total = n_layers * n_ex
    summed = total - n_ex
    pos = place()
    core, partner = pos[0], pos[5]
    enter(pos[3:])
    ex = Exchange(pos, part, cot, got1, got2, sems, n_ex, 4)

    def layer_of(k):
        return n_layers - 1 - lax.div(k, n_ex)

    def weight_copies(layer):
        near = [
            pltpu.make_async_copy(w_down.at[layer], w2.at[layer, pl.ds(0, d_ff)], w_sems.at[0, layer, 0]),
            pltpu.make_async_copy(w_up.at[layer], w1.at[layer, :, pl.ds(0, d_ff)], w_sems.at[0, layer, 1]),
        ]
        far = [
            push(w_down.at[layer], w2.at[layer, pl.ds(d_ff, d_ff)], w_sems.at[1, layer, 0], w_sems.at[2, layer, 0], partner),
            push(w_up.at[layer], w1.at[layer, :, pl.ds(d_ff, d_ff)], w_sems.at[1, layer, 1], w_sems.at[2, layer, 1], partner),
        ]
        return near, far

    def far_copy(g):
        first = lax.rem(g, groups) * U_GROUP
        layer = n_layers - 1 - lax.div(g, groups)
        return push(u.at[layer, 1 - core, pl.ds(first, U_GROUP)], u_far.at[pl.ds(g * U_GROUP, U_GROUP)], u_sems.at[0, g], u_sems.at[1, g], partner)

    def cot_copy(e):
        return pltpu.make_async_copy(d_out.at[core, e], cot.at[e], cot_sems.at[e])

    def load_copies(k):
        layer, e, s = layer_of(k), lax.rem(k, n_ex), lax.rem(k, 2)
        return [
            pltpu.make_async_copy(u.at[layer, core, e], u_own.at[s], load_sems.at[s, 0]),
            pltpu.make_async_copy(x.at[layer, core, e], x_buf.at[s], load_sems.at[s, 1]),
        ]

    def dh_copies(k):
        layer, e, s = layer_of(k), lax.rem(k, n_ex), lax.rem(k, 2)
        near = pltpu.make_async_copy(dh.at[s, :, pl.ds(0, d_ff)], dh_out.at[layer, core, e], dh_sems.at[s, 0])
        far = push(dh.at[s, :, pl.ds(d_ff, d_ff)], dh_out.at[layer, core, e], dh_sems.at[s, 1], all_sems.at[0], partner)
        return near, far

    def dx_copies(j):
        step, e, s = lax.div(j, n_ex), lax.rem(j, n_ex), lax.rem(j, 4)
        near = pltpu.make_async_copy(cot.at[e], dx_out.at[step, core, e], dx_sems.at[s, 0])
        far = push(cot.at[e], dx_out.at[step, core, e], dx_sems.at[s, 1], all_sems.at[1], partner)
        return near, far

    def part_copy(k):
        s = lax.rem(k, 4)
        return pltpu.make_async_copy(part.at[s], part_out.at[lax.rem(k, n_ex)], part_sems.at[s])

    def save(j):
        for copy in dx_copies(j):
            copy.start()

    def saved(j):
        near, far = dx_copies(j)
        near.wait()
        far.wait_send()

    top = n_layers - 1
    near, far = weight_copies(top)
    near[0].start()
    far[0].start()
    far_copy(0).start()
    cot_copy(0).start()
    for copy in load_copies(0):
        copy.start()
    near[1].start()
    far[1].start()

    @pl.loop(1, n_ex)
    def _(e):
        cot_copy(e).start()

    for layer in reversed(range(top)):
        for copy in sum(weight_copies(layer), []):
            copy.start()

    @pl.loop(1, n_layers * groups)
    def _(g):
        far_copy(g).start()

    norm_out[...] = jnp.zeros_like(norm_out)

    def compute(k):
        layer, e, s = layer_of(k), lax.rem(k, n_ex), lax.rem(k, 2)

        @pl.when(lax.rem(k, n_ex) == 0)
        def _():
            near, far = weight_copies(layer)
            for copy in near:
                copy.wait()
            for copy in far:
                copy.wait_recv()

        @pl.when(lax.rem(k, U_GROUP) == 0)
        def _():
            far_copy(lax.div(k, U_GROUP)).wait_recv()

        @pl.when(k < n_ex)
        def _():
            cot_copy(e).wait()

        for copy in load_copies(k):
            copy.wait()

        @pl.when(k + 1 < total)
        def _():
            for copy in load_copies(k + 1):
                copy.start()

        @pl.when(k >= 2)
        def _():
            near, far = dh_copies(k - 2)
            near.wait()
            far.wait_send()

        d_act[...] = lax.dot_general(cot[e].reshape(seq, d_model), w2[layer], NT, preferred_element_type=F32)
        rows = 32

        @pl.loop(0, seq // rows)
        def _(r):
            at = pl.ds(pl.multiple_of(r * rows, rows), rows)
            for half in range(2):
                columns = pl.ds(half * d_ff, d_ff)
                v = (u_own[s, at] if half == 0 else u_far[k, at]).astype(F32)
                square = v * v
                t = jnp.tanh(COEF * (v + CUBE * (square * v)))
                gate = 0.5 * (1.0 + t)
                slope = gate + (0.5 * v) * (1.0 - t * t) * (COEF * (1.0 + (3.0 * CUBE) * square))
                hid[at, columns] = (v * gate).astype(BF16)
                dh[s, at, columns] = (slope * d_act[at, columns]).astype(BF16)

        for copy in dh_copies(k):
            copy.start()
        back = lax.dot_general(dh[s], w1[layer], NT, preferred_element_type=F32)
        part[lax.rem(k, 4)] = back.astype(BF16).reshape(pieces)

        @pl.when(k < summed)
        def _():
            ex.start(0, k)

        @pl.when(k >= summed)
        def _():
            part_copy(k).start()

        for left, right in ((hid[...], cot[e].reshape(seq, d_model)), (x_buf[s], dh[s])):
            gram_a[...] = lax.dot_general(left, left, NT, preferred_element_type=F32)
            gram_b[...] = lax.dot_general(right, right, NT, preferred_element_type=F32)
            norm_out[e] += jnp.sum((gram_a[...] * gram_b[...]).reshape(seq // 8, 8, seq), axis=0)

    def iteration(k):
        run_stages(ex, k, summed, save, saved)

        @pl.when(jnp.logical_and(k >= summed + LAG, k < total + LAG))
        def _():
            part_copy(k - LAG).wait()

        @pl.when(k < total)
        def _():
            compute(k)

    @pl.loop(0, max(total + LAG, summed + 5 * LAG))
    def _(k):
        iteration(k)

    for k in (total - 2, total - 1):
        near, far = dh_copies(k)
        near.wait()
        far.wait_send()
    pltpu.make_async_copy(dh_out.at[:, 1 - core], dh_out.at[:, 1 - core], all_sems.at[0]).wait()
    pltpu.make_async_copy(dx_out.at[:, 1 - core], dx_out.at[:, 1 - core], all_sems.at[1]).wait()
    for layer in range(n_layers):
        for copy in weight_copies(layer)[1]:
            copy.wait_send()

    @pl.loop(0, n_layers * groups)
    def _(g):
        far_copy(g).wait_send()


def backward_call(u, x, w_up, w_down, d_out):
    n_layers, _, n_ex, seq, d_ff = u.shape
    d_model = x.shape[-1]
    pieces = (8, seq // 8, d_model)
    total = n_layers * n_ex
    rows = total * seq
    dma = pltpu.SemaphoreType.DMA
    return pl.pallas_call(
        backward_kernel,
        out_shape=(
            jax.ShapeDtypeStruct((n_layers - 1, 2, n_ex) + pieces, BF16),
            jax.ShapeDtypeStruct((n_layers, 2, n_ex, seq, d_ff), BF16),
            jax.ShapeDtypeStruct((n_ex,) + pieces, BF16),
            jax.ShapeDtypeStruct((n_ex, 8, seq), F32),
        ),
        in_specs=[ANY] * 5,
        out_specs=(ANY, ANY, ANY, VMEM),
        scratch_shapes=[
            pltpu.VMEM((n_ex,) + pieces, BF16),
            pltpu.VMEM((n_layers, d_model, 2 * d_ff), BF16),
            pltpu.VMEM((n_layers, 2 * d_ff, d_model), BF16),
            pltpu.VMEM((2, seq, d_ff), BF16),
            pltpu.VMEM((total, seq, d_ff), BF16),
            pltpu.VMEM((2, seq, d_model), BF16),
            pltpu.VMEM((seq, 2 * d_ff), F32),
            pltpu.VMEM((seq, 2 * d_ff), BF16),
            pltpu.VMEM((2, seq, 2 * d_ff), BF16),
            pltpu.VMEM((4,) + pieces, BF16),
            pltpu.VMEM((4, 2, 2) + pieces[1:], BF16),
            pltpu.VMEM((4, 2) + pieces[1:], BF16),
            pltpu.VMEM((seq, seq), F32),
            pltpu.VMEM((seq, seq), F32),
            dma((2, 4, 4, 2)),
            dma((3, n_layers, 2)),
            dma((2, total // U_GROUP)),
            dma((n_ex,)),
            dma((2, 2)),
            dma((2, 2)),
            dma((4, 2)),
            dma((2,)),
            dma((4,)),
        ],
        compiler_params=pltpu.CompilerParams(collective_id=0, has_side_effects=True, vmem_limit_bytes=66_000_000),
        cost_estimate=pl.CostEstimate(flops=rows * d_model * d_ff * 16, bytes_accessed=rows * d_model * 16, transcendentals=rows * d_ff * 2),
        name="backward",
    )(u, x, w_up, w_down, d_out.reshape((2, n_ex) + pieces))


def sum_kernel(part_in, cot_in, dx_out, cot, part, got1, got2, sems, in_sems, dx_sems, all_sems):
    n_ex = part_in.shape[0]
    pos = place()
    core, partner = pos[0], pos[5]
    enter(pos[3:])
    ex = Exchange(pos, part, cot, got1, got2, sems, n_ex, n_ex)

    def in_copies(e):
        return [
            pltpu.make_async_copy(part_in.at[e], part.at[e], in_sems.at[e, 0]),
            pltpu.make_async_copy(cot_in.at[core, e], cot.at[e], in_sems.at[e, 1]),
        ]

    def dx_copies(j):
        s = lax.rem(j, 4)
        near = pltpu.make_async_copy(cot.at[j], dx_out.at[core, j], dx_sems.at[s, 0])
        far = push(cot.at[j], dx_out.at[core, j], dx_sems.at[s, 1], all_sems.at[0], partner)
        return near, far

    def save(j):
        for copy in dx_copies(j):
            copy.start()

    def saved(j):
        near, far = dx_copies(j)
        near.wait()
        far.wait_send()

    @pl.loop(0, n_ex)
    def _(e):
        for copy in in_copies(e):
            copy.start()

    @pl.loop(0, n_ex + 5 * LAG)
    def _(k):
        run_stages(ex, k, n_ex, save, saved)

        @pl.when(k < n_ex)
        def _():
            for copy in in_copies(k):
                copy.wait()
            ex.start(0, k)

    pltpu.make_async_copy(dx_out.at[1 - core], dx_out.at[1 - core], all_sems.at[0]).wait()


def sum_call(part, cot):
    n_ex = part.shape[0]
    pieces = part.shape[1:]
    dma = pltpu.SemaphoreType.DMA
    return pl.pallas_call(
        sum_kernel,
        out_shape=jax.ShapeDtypeStruct((2, n_ex) + pieces, BF16),
        in_specs=[ANY] * 2,
        out_specs=ANY,
        scratch_shapes=[
            pltpu.VMEM((n_ex,) + pieces, BF16),
            pltpu.VMEM((n_ex,) + pieces, BF16),
            pltpu.VMEM((4, 2, 2) + pieces[1:], BF16),
            pltpu.VMEM((4, 2) + pieces[1:], BF16),
            dma((2, 4, 4, 2)),
            dma((n_ex, 2)),
            dma((4, 2)),
            dma((1,)),
        ],
        compiler_params=pltpu.CompilerParams(collective_id=1, has_side_effects=True, vmem_limit_bytes=40_000_000),
        cost_estimate=pl.CostEstimate(flops=200_000_000_000, bytes_accessed=part.size * 8, transcendentals=0),
        name="sum_rows",
    )(part, cot)


def solution(mesh):
    dp_size = mesh.shape["dp"]

    def local_pass(x_in, u_pre, w_up, w_down, d_out, noise_up, noise_down, clip_norm, noise_mult):
        n_layers = x_in.shape[0]
        examples = d_out.shape[0] * d_out.shape[1] * dp_size
        core = lax.rem(lax.axis_index("tp"), 2)
        dx, dh, part, norms = backward_call(u_pre, x_in, w_up, w_down, d_out)
        own_norm = jnp.sum(norms, axis=(1, 2))
        norm_part = jnp.where(jnp.arange(2)[:, None] == core, own_norm[None, :], 0.0)
        norm_vec = lax.psum(norm_part, "tp")
        clip_col = jnp.minimum(1.0, clip_norm[0] / jnp.sqrt(norm_vec))[:, :, None, None]
        noise_scale = noise_mult[0] * clip_norm[0]
        up_parts, down_parts = [], []
        for layer_idx in range(n_layers):
            if layer_idx == n_layers - 1:
                cot_layer = d_out
            else:
                cot_layer = dx[n_layers - 2 - layer_idx].reshape(d_out.shape)
            hidden = jax.nn.gelu(u_pre[layer_idx].astype(F32)).astype(BF16)
            scaled_dh = (dh[layer_idx] * clip_col).astype(BF16)
            scaled_cot = (cot_layer * clip_col).astype(BF16)
            up_parts.append(jnp.einsum("mbtd,mbtn->dn", x_in[layer_idx], scaled_dh, preferred_element_type=F32))
            down_parts.append(jnp.einsum("mbtn,mbtd->nd", hidden, scaled_cot, preferred_element_type=F32))
        late_part, _ = lax.optimization_barrier((part, (up_parts, down_parts)))
        d_in = sum_call(late_part, dx[n_layers - 2]).reshape(d_out.shape)
        up_grads, down_grads = [], []
        for layer_idx in range(n_layers):
            up_sum = lax.psum_scatter(up_parts[layer_idx], "dp", scatter_dimension=0, tiled=True)
            down_sum = lax.psum_scatter(down_parts[layer_idx], "dp", scatter_dimension=1, tiled=True)
            up_grads.append((up_sum + noise_scale * noise_up[layer_idx]) / examples)
            down_grads.append((down_sum + noise_scale * noise_down[layer_idx]) / examples)
        return jnp.stack(up_grads), jnp.stack(down_grads), d_in

    in_specs = (P(None, None, "dp", None, None), P(None, None, "dp", None, "tp"), P(None, None, "tp"), P(None, "tp", None), P(None, "dp", None, None), P(None, "dp", "tp"), P(None, "tp", "dp"), P(), P())
    out_specs = (P(None, "dp", "tp"), P(None, "tp", "dp"), P(None, "dp", None, None))
    return jax.shard_map(local_pass, mesh=mesh, in_specs=in_specs, out_specs=out_specs, check_vma=False)
```

```python
import functools
import math

import jax
import jax.numpy as jnp
from jax import lax
from jax.experimental import pallas as pl
from jax.experimental.pallas import tpu as pltpu
from jax.sharding import PartitionSpec as P

F32 = jnp.float32
BF16 = jnp.bfloat16
NT = (((1,), (1,)), ((), ()))
ANY = pl.BlockSpec(memory_space=pl.ANY)
VMEM = pl.BlockSpec(memory_space=pltpu.VMEM)
LAG = 1
U_GROUP = 4
COEF = math.sqrt(2.0 / math.pi)
CUBE = 0.044715


def place():
    t = lax.axis_index("tp")
    core = lax.rem(t, 2)
    px = lax.rem(lax.div(t, 2), 2)
    py = lax.div(t, 4)
    return core, px, py, t + 2 - 4 * px, t + 4 - 8 * py, t + 1 - 2 * core


def enter(peers):
    barrier = pltpu.get_barrier_semaphore()
    for peer in peers:
        pl.semaphore_signal(barrier, inc=1, device_id={"tp": peer}, device_id_type=pl.DeviceIdType.MESH)
    pl.semaphore_wait(barrier, len(peers))


def push(src, dst, send_sem, recv_sem, peer):
    return pltpu.make_async_remote_copy(src_ref=src, dst_ref=dst, send_sem=send_sem, recv_sem=recv_sem, device_id={"tp": peer}, device_id_type=pl.DeviceIdType.MESH)


class Exchange:
    def __init__(self, pos, part, cot, got1, got2, sems, n_examples, n_slots):
        self.core, self.px, self.py, self.nx, self.ny, self.partner = pos
        self.part, self.cot, self.got1, self.got2, self.sems = part, cot, got1, got2, sems
        self.n_examples, self.n_slots = n_examples, n_slots

    def copies(self, kind, j):
        px, py = self.px, self.py
        part = self.part.at[lax.rem(j, self.n_slots)]
        cot = self.cot.at[lax.rem(j, self.n_examples)]
        s = lax.rem(j, 4)
        send, recv = self.sems.at[0, kind], self.sems.at[1, kind]
        if kind == 0:
            pairs = ((part.at[pl.ds(2 * (1 - px), 2)], self.got1.at[s, 0], self.nx), (part.at[pl.ds(4 + 2 * (1 - py), 2)], self.got1.at[s, 1], self.ny))
        elif kind == 1:
            pairs = ((part.at[2 * px + 1 - py], self.got2.at[s, 0], self.ny), (part.at[4 + 2 * py + 1 - px], self.got2.at[s, 1], self.nx))
        elif kind == 2:
            own_a, own_b = cot.at[2 * px + py], cot.at[4 + 2 * py + px]
            pairs = ((own_a, own_a, self.ny), (own_b, own_b, self.nx))
        else:
            two_a, two_b = cot.at[pl.ds(2 * px, 2)], cot.at[pl.ds(4 + 2 * py, 2)]
            pairs = ((two_a, two_a, self.nx), (two_b, two_b, self.ny))
        return [push(src, dst, send.at[s, c], recv.at[s, c], peer) for c, (src, dst, peer) in enumerate(pairs)]

    def start(self, kind, j):
        for copy in self.copies(kind, j):
            copy.start()

    def wait(self, kind, j):
        for copy in self.copies(kind, j):
            copy.wait()

    def add_first(self, j):
        self.wait(0, j)
        slot, s = lax.rem(j, self.n_slots), lax.rem(j, 4)
        for c, first in enumerate((2 * self.px, 4 + 2 * self.py)):
            for i in range(2):
                mine = self.part[slot, first + i].astype(F32) + self.got1[s, c, i].astype(F32)
                self.part[slot, first + i] = mine.astype(BF16)
        self.start(1, j)

    def add_second(self, j):
        self.wait(1, j)
        slot, s, e = lax.rem(j, self.n_slots), lax.rem(j, 4), lax.rem(j, self.n_examples)
        for c, own in enumerate((2 * self.px + self.py, 4 + 2 * self.py + self.px)):
            back = self.part[slot, own].astype(F32) + self.got2[s, c].astype(F32)
            self.cot[e, own] = (self.cot[e, own].astype(F32) + back).astype(BF16)
        self.start(2, j)

    def forward(self, j):
        self.wait(2, j)
        self.start(3, j)


def run_stages(ex, k, count, save, saved):
    def at(lag, fn):
        j = k - lag * LAG

        @pl.when(jnp.logical_and(j >= 0, j < count))
        def _():
            fn(j)

    def finish(j):
        ex.wait(3, j)
        save(j)

    at(5, saved)
    at(4, finish)
    at(3, ex.forward)
    at(2, ex.add_second)
    at(1, ex.add_first)


def backward_kernel(u, x, w_up, w_down, d_out, dx_out, dh_out, part_out, norm_out, cot, w1, w2, u_own, u_far, x_buf, d_act, hid, dh, part, got1, got2, gram_a, gram_b, sems, w_sems, u_sems, cot_sems, load_sems, dh_sems, dx_sems, all_sems, part_sems):
    n_layers, _, n_ex, seq, d_ff = u.shape
    d_model = x.shape[-1]
    pieces = cot.shape[1:]
    groups = n_ex // U_GROUP
    total = n_layers * n_ex
    summed = total - n_ex
    pos = place()
    core, partner = pos[0], pos[5]
    enter(pos[3:])
    ex = Exchange(pos, part, cot, got1, got2, sems, n_ex, 4)

    def layer_of(k):
        return n_layers - 1 - lax.div(k, n_ex)

    def weight_copies(layer):
        near = [
            pltpu.make_async_copy(w_down.at[layer], w2.at[layer, pl.ds(0, d_ff)], w_sems.at[0, layer, 0]),
            pltpu.make_async_copy(w_up.at[layer], w1.at[layer, :, pl.ds(0, d_ff)], w_sems.at[0, layer, 1]),
        ]
        far = [
            push(w_down.at[layer], w2.at[layer, pl.ds(d_ff, d_ff)], w_sems.at[1, layer, 0], w_sems.at[2, layer, 0], partner),
            push(w_up.at[layer], w1.at[layer, :, pl.ds(d_ff, d_ff)], w_sems.at[1, layer, 1], w_sems.at[2, layer, 1], partner),
        ]
        return near, far

    def far_copy(g):
        first = lax.rem(g, groups) * U_GROUP
        layer = n_layers - 1 - lax.div(g, groups)
        return push(u.at[layer, 1 - core, pl.ds(first, U_GROUP)], u_far.at[pl.ds(g * U_GROUP, U_GROUP)], u_sems.at[0, g], u_sems.at[1, g], partner)

    def cot_copy(e):
        return pltpu.make_async_copy(d_out.at[core, e], cot.at[e], cot_sems.at[e])

    def load_copies(p):
        k, s = example_at(p), lax.rem(p, 2)
        layer, e = layer_of(k), lax.rem(k, n_ex)
        return [
            pltpu.make_async_copy(u.at[layer, core, e], u_own.at[s], load_sems.at[s, 0]),
            pltpu.make_async_copy(x.at[layer, core, e], x_buf.at[s], load_sems.at[s, 1]),
        ]

    def dh_copies(p):
        k, s = example_at(p), lax.rem(p, 2)
        layer, e = layer_of(k), lax.rem(k, n_ex)
        near = pltpu.make_async_copy(dh.at[s, :, pl.ds(0, d_ff)], dh_out.at[layer, core, e], dh_sems.at[s, 0])
        far = push(dh.at[s, :, pl.ds(d_ff, d_ff)], dh_out.at[layer, core, e], dh_sems.at[s, 1], all_sems.at[0], partner)
        return near, far

    def dx_copies(j):
        step, e, s = lax.div(j, n_ex), lax.rem(j, n_ex), lax.rem(j, 4)
        near = pltpu.make_async_copy(cot.at[e], dx_out.at[step, core, e], dx_sems.at[s, 0])
        far = push(cot.at[e], dx_out.at[step, core, e], dx_sems.at[s, 1], all_sems.at[1], partner)
        return near, far

    def part_copy(k):
        s = lax.rem(k, 2)
        return pltpu.make_async_copy(part.at[4 + s], part_out.at[lax.rem(k, n_ex)], part_sems.at[s])

    early = summed - n_ex + 4 * LAG + 1

    def first_of(i):
        return jnp.where(i <= early, i, jnp.where(i < summed, 2 * i - early, i + summed - early))

    def example_at(p):
        r = p - early
        half = lax.div(r, 2)
        mixed = jnp.where(lax.rem(r, 2) == 0, early + half, summed + half)
        return jnp.where(jnp.logical_or(r < 0, p >= 2 * summed - early), p, mixed)

    def save(j):
        for copy in dx_copies(j):
            copy.start()

    def saved(j):
        near, far = dx_copies(j)
        near.wait()
        far.wait_send()

    top = n_layers - 1
    near, far = weight_copies(top)
    near[0].start()
    far[0].start()
    far_copy(0).start()
    cot_copy(0).start()
    for copy in load_copies(0):
        copy.start()
    near[1].start()
    far[1].start()

    @pl.loop(1, n_ex)
    def _(e):
        cot_copy(e).start()

    for layer in reversed(range(top)):
        for copy in sum(weight_copies(layer), []):
            copy.start()

    @pl.loop(1, n_layers * groups)
    def _(g):
        far_copy(g).start()

    norm_out[...] = jnp.zeros_like(norm_out)

    def compute(p):
        k, s = example_at(p), lax.rem(p, 2)
        layer, e = layer_of(k), lax.rem(k, n_ex)

        @pl.when(lax.rem(k, n_ex) == 0)
        def _():
            near, far = weight_copies(layer)
            for copy in near:
                copy.wait()
            for copy in far:
                copy.wait_recv()

        @pl.when(lax.rem(k, U_GROUP) == 0)
        def _():
            far_copy(lax.div(k, U_GROUP)).wait_recv()

        @pl.when(k < n_ex)
        def _():
            cot_copy(e).wait()

        for copy in load_copies(p):
            copy.wait()

        @pl.when(p + 1 < total)
        def _():
            for copy in load_copies(p + 1):
                copy.start()

        @pl.when(p >= 2)
        def _():
            near, far = dh_copies(p - 2)
            near.wait()
            far.wait_send()

        @pl.when(k >= summed + 2)
        def _():
            part_copy(k - 2).wait()

        d_act[...] = lax.dot_general(cot[e].reshape(seq, d_model), w2[layer], NT, preferred_element_type=F32)
        rows = 32

        @pl.loop(0, seq // rows)
        def _(r):
            at = pl.ds(pl.multiple_of(r * rows, rows), rows)
            for half in range(2):
                columns = pl.ds(half * d_ff, d_ff)
                v = (u_own[s, at] if half == 0 else u_far[k, at]).astype(F32)
                square = v * v
                t = jnp.tanh(COEF * (v + CUBE * (square * v)))
                gate = 0.5 * (1.0 + t)
                slope = gate + (0.5 * v) * (1.0 - t * t) * (COEF * (1.0 + (3.0 * CUBE) * square))
                hid[at, columns] = (v * gate).astype(BF16)
                dh[s, at, columns] = (slope * d_act[at, columns]).astype(BF16)

        for copy in dh_copies(p):
            copy.start()
        back = lax.dot_general(dh[s], w1[layer], NT, preferred_element_type=F32)
        part[jnp.where(k < summed, lax.rem(k, 4), 4 + lax.rem(k, 2))] = back.astype(BF16).reshape(pieces)

        @pl.when(k < summed)
        def _():
            ex.start(0, k)

        @pl.when(k >= summed)
        def _():
            part_copy(k).start()

        for left, right in ((hid[...], cot[e].reshape(seq, d_model)), (x_buf[s], dh[s])):
            gram_a[...] = lax.dot_general(left, left, NT, preferred_element_type=F32)
            gram_b[...] = lax.dot_general(right, right, NT, preferred_element_type=F32)
            norm_out[e] += jnp.sum((gram_a[...] * gram_b[...]).reshape(seq // 8, 8, seq), axis=0)

    @pl.loop(0, summed + 5 * LAG)
    def _(i):
        run_stages(ex, i, summed, save, saved)

        @pl.loop(first_of(i), first_of(i + 1))
        def _(p):
            compute(p)

    for k in (total - 2, total - 1):
        part_copy(k).wait()
    for k in (total - 2, total - 1):
        near, far = dh_copies(k)
        near.wait()
        far.wait_send()
    pltpu.make_async_copy(dh_out.at[:, 1 - core], dh_out.at[:, 1 - core], all_sems.at[0]).wait()
    pltpu.make_async_copy(dx_out.at[:, 1 - core], dx_out.at[:, 1 - core], all_sems.at[1]).wait()
    for layer in range(n_layers):
        for copy in weight_copies(layer)[1]:
            copy.wait_send()

    @pl.loop(0, n_layers * groups)
    def _(g):
        far_copy(g).wait_send()


def backward_call(u, x, w_up, w_down, d_out):
    n_layers, _, n_ex, seq, d_ff = u.shape
    d_model = x.shape[-1]
    pieces = (8, seq // 8, d_model)
    total = n_layers * n_ex
    rows = total * seq
    dma = pltpu.SemaphoreType.DMA
    return pl.pallas_call(
        backward_kernel,
        out_shape=(
            jax.ShapeDtypeStruct((n_layers - 1, 2, n_ex) + pieces, BF16),
            jax.ShapeDtypeStruct((n_layers, 2, n_ex, seq, d_ff), BF16),
            jax.ShapeDtypeStruct((n_ex,) + pieces, BF16),
            jax.ShapeDtypeStruct((n_ex, 8, seq), F32),
        ),
        in_specs=[ANY] * 5,
        out_specs=(ANY, ANY, ANY, VMEM),
        scratch_shapes=[
            pltpu.VMEM((n_ex,) + pieces, BF16),
            pltpu.VMEM((n_layers, d_model, 2 * d_ff), BF16),
            pltpu.VMEM((n_layers, 2 * d_ff, d_model), BF16),
            pltpu.VMEM((2, seq, d_ff), BF16),
            pltpu.VMEM((total, seq, d_ff), BF16),
            pltpu.VMEM((2, seq, d_model), BF16),
            pltpu.VMEM((seq, 2 * d_ff), F32),
            pltpu.VMEM((seq, 2 * d_ff), BF16),
            pltpu.VMEM((2, seq, 2 * d_ff), BF16),
            pltpu.VMEM((6,) + pieces, BF16),
            pltpu.VMEM((4, 2, 2) + pieces[1:], BF16),
            pltpu.VMEM((4, 2) + pieces[1:], BF16),
            pltpu.VMEM((seq, seq), F32),
            pltpu.VMEM((seq, seq), F32),
            dma((2, 4, 4, 2)),
            dma((3, n_layers, 2)),
            dma((2, total // U_GROUP)),
            dma((n_ex,)),
            dma((2, 2)),
            dma((2, 2)),
            dma((4, 2)),
            dma((2,)),
            dma((2,)),
        ],
        compiler_params=pltpu.CompilerParams(collective_id=0, has_side_effects=True, vmem_limit_bytes=66_000_000),
        cost_estimate=pl.CostEstimate(flops=rows * d_model * d_ff * 16, bytes_accessed=rows * d_model * 16, transcendentals=rows * d_ff * 2),
        name="backward",
    )(u, x, w_up, w_down, d_out.reshape((2, n_ex) + pieces))


def gelu(v):
    return v * (0.5 * (1.0 + jnp.tanh(COEF * (v + CUBE * (v * v * v)))))


class Ring:
    def __init__(self, size, sums, got, sems, out):
        z = lax.axis_index("dp")
        self.z, self.size = z, size
        self.peers = lax.rem(z + 1, size), lax.rem(z + size - 1, size)
        self.sums, self.got, self.sems, self.out = sums, got, sems, out

    def tile(self, step, way):
        if way == 0:
            return 2 * lax.rem(self.z + 2 * self.size - 1 - step, self.size)
        return 2 * lax.rem(self.z + 1 + step, self.size) + 1

    def copies(self, step, j):
        s = lax.rem(j, 4)
        block = self.sums.at[lax.rem(lax.div(j, 4), 3), lax.rem(j, 4)]
        return [
            pltpu.make_async_remote_copy(
                src_ref=block.at[self.tile(step, way)],
                dst_ref=self.got.at[step, s, way],
                send_sem=self.sems.at[0, step, s, way],
                recv_sem=self.sems.at[1, step, s, way],
                device_id={"dp": self.peers[way]},
                device_id_type=pl.DeviceIdType.MESH,
            )
            for way in range(2)
        ]

    def start(self, step, j):
        for copy in self.copies(step, j):
            copy.start()

    def add(self, step, j):
        for copy in self.copies(step, j):
            copy.wait()
        g, q, s = lax.div(j, 4), lax.rem(j, 4), lax.rem(j, 4)
        for way in range(2):
            at = lax.rem(g, 3), q, self.tile(step + 1, way)
            total = self.sums[at] + self.got[step, s, way]
            if step + 1 < self.size - 1:
                self.sums[at] = total
            else:
                rows, columns = total.shape
                self.out[g, pl.ds(pl.multiple_of(q * rows, rows), rows), pl.ds(way * columns, columns)] = total
        if step + 1 < self.size - 1:
            self.start(step + 1, j)


def gradient_kernel(size, part_in, dx_in, d_out, x, dh, u, clip, d_in, grads, cot, part, got1, got2, sums, got_z, a_buf, b_buf, a_scaled, b_scaled, sems, in_sems, dx_sems, all_sems, z_sems, load_sems):
    n_layers, _, n_ex, seq, d_ff = u.shape
    d_model = x.shape[-1]
    pairs = n_ex // 2
    per_grad = 2 * pairs
    per_step = per_grad // 4
    n_grads = 2 * n_layers
    steps = n_grads * per_grad
    last = n_layers - 2
    pos = place()
    core, partner = pos[0], pos[5]
    ring = Ring(size, sums, got_z, z_sems, grads)
    barrier = pltpu.get_barrier_semaphore()
    for peer in pos[3:]:
        pl.semaphore_signal(barrier, inc=1, device_id={"tp": peer}, device_id_type=pl.DeviceIdType.MESH)
    if size > 1:
        for peer in ring.peers:
            pl.semaphore_signal(barrier, inc=1, device_id={"dp": peer}, device_id_type=pl.DeviceIdType.MESH)
    pl.semaphore_wait(barrier, 5 if size > 1 else 3)
    ex = Exchange(pos, part, cot, got1, got2, sems, n_ex, n_ex)

    def in_copies(e):
        return [
            pltpu.make_async_copy(part_in.at[e], part.at[e], in_sems.at[e, 0]),
            pltpu.make_async_copy(dx_in.at[last, core, e], cot.at[e], in_sems.at[e, 1]),
        ]

    def dx_copies(j):
        s = lax.rem(j, 4)
        near = pltpu.make_async_copy(cot.at[j], d_in.at[core, j], dx_sems.at[s, 0])
        far = push(cot.at[j], d_in.at[core, j], dx_sems.at[s, 1], all_sems.at[0], partner)
        return near, far

    def save(j):
        for copy in dx_copies(j):
            copy.start()

    def saved(j):
        near, far = dx_copies(j)
        near.wait()
        far.wait_send()

    def where_is(t):
        g, pair = lax.div(t, per_grad), lax.rem(t, per_grad)
        return g, lax.rem(g, n_layers), lax.div(pair, pairs), 2 * lax.rem(pair, pairs), lax.rem(t, 2)

    def load(t):
        g, layer, m, e, s = where_is(t)
        two = pl.ds(e, 2)

        @pl.when(g < n_layers)
        def _():
            pltpu.make_async_copy(x.at[layer, m, two], a_buf.at[s], load_sems.at[s, 0]).start()
            pltpu.make_async_copy(dh.at[layer, m, two], b_buf.at[s], load_sems.at[s, 1]).start()

        @pl.when(g >= n_layers)
        def _():
            pltpu.make_async_copy(u.at[layer, m, two], b_buf.at[s], load_sems.at[s, 1]).start()

        @pl.when(g == n_grads - 1)
        def _():
            pltpu.make_async_copy(d_out.at[m, two], a_buf.at[s], load_sems.at[s, 0]).start()

        @pl.when(jnp.logical_and(g >= n_layers, g < n_grads - 1))
        def _():
            pltpu.make_async_copy(dx_in.at[last - layer, m, two], a_buf.at[s], load_sems.at[s, 0]).start()

    def accumulate(t):
        g, layer, m, e, s = where_is(t)

        @pl.when(t + 1 < steps)
        def _():
            load(t + 1)

        pltpu.make_async_copy(x.at[0, 0, pl.ds(0, 2)], a_buf.at[s], load_sems.at[s, 0]).wait()
        pltpu.make_async_copy(u.at[0, 0, pl.ds(0, 2)], b_buf.at[s], load_sems.at[s, 1]).wait()
        slot = lax.rem(g, 3)

        def add(b, a):
            c = lax.dot_general(b, a, (((0,), (0,)), ((), ())), preferred_element_type=F32)
            tiles, _, rows, columns = sums.shape[1:]
            first = lax.rem(t, per_grad) == 0
            for n in range(2 * size):
                new = c[:, n * columns:(n + 1) * columns].reshape(tiles, rows, columns)
                old = jnp.where(first, 0.0, sums[slot, :, n])
                sums[slot, :, n] = old + new

        @pl.when(g < n_layers)
        def _():
            for i in range(2):
                b_scaled[i * seq:(i + 1) * seq] = (b_buf[s, i].astype(F32) * clip[m * n_ex + e + i]).astype(BF16)
            add(b_scaled[...], a_buf[s].reshape(2 * seq, d_model))

        @pl.when(g >= n_layers)
        def _():
            for i in range(2):
                a_scaled[i * seq:(i + 1) * seq] = (a_buf[s, i].reshape(seq, d_model).astype(F32) * clip[m * n_ex + e + i]).astype(BF16)
                b_scaled[i * seq:(i + 1) * seq] = gelu(b_buf[s, i].astype(F32)).astype(BF16)
            add(b_scaled[...], a_scaled[...])

    load(0)

    @pl.loop(0, n_ex)
    def _(e):
        for copy in in_copies(e):
            copy.start()

    blocks = 4 * n_grads

    @pl.loop(0, max(blocks + 4 + size - 1, 2 * (n_ex + 5 * LAG)))
    def _(i):
        j = i - 4
        for step in reversed(range(size)):
            @pl.when(jnp.logical_and(j - step >= 0, j - step < blocks))
            def _(step=step):
                if step == 0:
                    ring.start(0, j)
                else:
                    ring.add(step - 1, j - step)

        @pl.when(lax.rem(i, 2) == 0)
        def _():
            k = lax.div(i, 2)

            @pl.when(k < n_ex)
            def _():
                for copy in in_copies(k):
                    copy.wait()
                ex.start(0, k)

            run_stages(ex, k, n_ex, save, saved)

        @pl.when(i < blocks)
        def _():
            @pl.loop(0, per_step)
            def _(r):
                accumulate(i * per_step + r)

    pltpu.make_async_copy(d_in.at[1 - core], d_in.at[1 - core], all_sems.at[0]).wait()


def gradient_call(size, part, dx, d_out, x, dh, u, clip):
    n_layers, _, n_ex, seq, d_ff = u.shape
    d_model = x.shape[-1]
    pieces = part.shape[1:]
    width = d_model // (2 * size)
    dma = pltpu.SemaphoreType.DMA
    return pl.pallas_call(
        functools.partial(gradient_kernel, size),
        out_shape=(
            jax.ShapeDtypeStruct((2, n_ex) + pieces, BF16),
            jax.ShapeDtypeStruct((2 * n_layers, d_ff, 2 * width), F32),
        ),
        in_specs=[ANY] * 6 + [pl.BlockSpec(memory_space=pltpu.SMEM)],
        out_specs=(ANY, VMEM),
        scratch_shapes=[
            pltpu.VMEM((n_ex,) + pieces, BF16),
            pltpu.VMEM((n_ex,) + pieces, BF16),
            pltpu.VMEM((4, 2, 2) + pieces[1:], BF16),
            pltpu.VMEM((4, 2) + pieces[1:], BF16),
            pltpu.VMEM((3, 4, 2 * size, d_ff // 4, width), F32),
            pltpu.VMEM((size - 1, 4, 2, d_ff // 4, width), F32),
            pltpu.VMEM((2, 2) + pieces, BF16),
            pltpu.VMEM((2, 2, seq, d_ff), BF16),
            pltpu.VMEM((2 * seq, d_model), BF16),
            pltpu.VMEM((2 * seq, d_ff), BF16),
            dma((2, 4, 4, 2)),
            dma((n_ex, 2)),
            dma((4, 2)),
            dma((1,)),
            dma((2, size - 1, 4, 2)),
            dma((2, 2)),
        ],
        compiler_params=pltpu.CompilerParams(collective_id=1, has_side_effects=True, vmem_limit_bytes=66_000_000),
        name="gradient",
    )(part, dx, d_out.reshape((2, n_ex) + pieces), x.reshape((n_layers, 2, n_ex) + pieces), dh, u, clip)


def solution(mesh):
    dp_size = mesh.shape["dp"]

    def local_pass(x_in, u_pre, w_up, w_down, d_out, noise_up, noise_down, clip_norm, noise_mult):
        n_layers = x_in.shape[0]
        examples = d_out.shape[0] * d_out.shape[1] * dp_size
        core = lax.rem(lax.axis_index("tp"), 2)
        dx, dh, part, norms = backward_call(u_pre, x_in, w_up, w_down, d_out)
        own_norm = jnp.sum(norms, axis=(1, 2))
        norm_part = jnp.where(jnp.arange(2)[:, None] == core, own_norm[None, :], 0.0)
        norm_vec = lax.psum(norm_part, "tp")
        clip_fac = jnp.minimum(1.0, clip_norm[0] / jnp.sqrt(norm_vec)).reshape(-1)
        noise_scale = noise_mult[0] * clip_norm[0]
        d_in, sums = gradient_call(dp_size, part, dx, d_out, x_in, dh, u_pre, clip_fac)
        up_sum = jnp.swapaxes(sums[:n_layers], 1, 2)
        down_sum = sums[n_layers:]
        up_grad = (up_sum + noise_scale * noise_up) / examples
        down_grad = (down_sum + noise_scale * noise_down) / examples
        return up_grad, down_grad, d_in.reshape(d_out.shape)

    in_specs = (P(None, None, "dp", None, None), P(None, None, "dp", None, "tp"), P(None, None, "tp"), P(None, "tp", None), P(None, "dp", None, None), P(None, "dp", "tp"), P(None, "tp", "dp"), P(), P())
    out_specs = (P(None, "dp", "tp"), P(None, "tp", "dp"), P(None, "dp", None, None))
    return jax.shard_map(local_pass, mesh=mesh, in_specs=in_specs, out_specs=out_specs, check_vma=False)
```

```python
import functools
import math

import jax
import jax.numpy as jnp
from jax import lax
from jax.experimental import pallas as pl
from jax.experimental.pallas import tpu as pltpu
from jax.sharding import PartitionSpec as P

F32 = jnp.float32
BF16 = jnp.bfloat16
NT = (((1,), (1,)), ((), ()))
ANY = pl.BlockSpec(memory_space=pl.ANY)
VMEM = pl.BlockSpec(memory_space=pltpu.VMEM)
LAG = 1
U_GROUP = 2
COEF = math.sqrt(2.0 / math.pi)
CUBE = 0.044715


def place():
    t = lax.axis_index("tp")
    core = lax.rem(t, 2)
    px = lax.rem(lax.div(t, 2), 2)
    py = lax.div(t, 4)
    return core, px, py, t + 2 - 4 * px, t + 4 - 8 * py, t + 1 - 2 * core


def enter(peers):
    barrier = pltpu.get_barrier_semaphore()
    for peer in peers:
        pl.semaphore_signal(barrier, inc=1, device_id={"tp": peer}, device_id_type=pl.DeviceIdType.MESH)
    pl.semaphore_wait(barrier, len(peers))


def push(src, dst, send_sem, recv_sem, peer):
    return pltpu.make_async_remote_copy(src_ref=src, dst_ref=dst, send_sem=send_sem, recv_sem=recv_sem, device_id={"tp": peer}, device_id_type=pl.DeviceIdType.MESH)


class Exchange:
    def __init__(self, pos, part, cot, got1, got2, sems, n_examples, n_slots):
        self.core, self.px, self.py, self.nx, self.ny, self.partner = pos
        self.part, self.cot, self.got1, self.got2, self.sems = part, cot, got1, got2, sems
        self.n_examples, self.n_slots = n_examples, n_slots

    def copies(self, kind, j):
        px, py = self.px, self.py
        part = self.part.at[lax.rem(j, self.n_slots)]
        cot = self.cot.at[lax.rem(j, self.n_examples)]
        s = lax.rem(j, 4)
        send, recv = self.sems.at[0, kind], self.sems.at[1, kind]
        if kind == 0:
            pairs = ((part.at[pl.ds(2 * (1 - px), 2)], self.got1.at[s, 0], self.nx), (part.at[pl.ds(4 + 2 * (1 - py), 2)], self.got1.at[s, 1], self.ny))
        elif kind == 1:
            pairs = ((part.at[2 * px + 1 - py], self.got2.at[s, 0], self.ny), (part.at[4 + 2 * py + 1 - px], self.got2.at[s, 1], self.nx))
        elif kind == 2:
            own_a, own_b = cot.at[2 * px + py], cot.at[4 + 2 * py + px]
            pairs = ((own_a, own_a, self.ny), (own_b, own_b, self.nx))
        else:
            two_a, two_b = cot.at[pl.ds(2 * px, 2)], cot.at[pl.ds(4 + 2 * py, 2)]
            pairs = ((two_a, two_a, self.nx), (two_b, two_b, self.ny))
        return [push(src, dst, send.at[s, c], recv.at[s, c], peer) for c, (src, dst, peer) in enumerate(pairs)]

    def start(self, kind, j):
        for copy in self.copies(kind, j):
            copy.start()

    def wait(self, kind, j):
        for copy in self.copies(kind, j):
            copy.wait()

    def add_first(self, j):
        self.wait(0, j)
        slot, s = lax.rem(j, self.n_slots), lax.rem(j, 4)
        for c, first in enumerate((2 * self.px, 4 + 2 * self.py)):
            for i in range(2):
                mine = self.part[slot, first + i].astype(F32) + self.got1[s, c, i].astype(F32)
                self.part[slot, first + i] = mine.astype(BF16)
        self.start(1, j)

    def add_second(self, j):
        self.wait(1, j)
        slot, s, e = lax.rem(j, self.n_slots), lax.rem(j, 4), lax.rem(j, self.n_examples)
        for c, own in enumerate((2 * self.px + self.py, 4 + 2 * self.py + self.px)):
            back = self.part[slot, own].astype(F32) + self.got2[s, c].astype(F32)
            self.cot[e, own] = (self.cot[e, own].astype(F32) + back).astype(BF16)
        self.start(2, j)

    def forward(self, j):
        self.wait(2, j)
        self.start(3, j)


def run_stages(ex, k, count, save, saved):
    def at(lag, fn):
        j = k - lag * LAG

        @pl.when(jnp.logical_and(j >= 0, j < count))
        def _():
            fn(j)

    def finish(j):
        ex.wait(3, j)
        save(j)

    at(5, saved)
    at(4, finish)
    at(3, ex.forward)
    at(2, ex.add_second)
    at(1, ex.add_first)


def backward_kernel(u, x, w_up, w_down, d_out, dx_out, dh_out, part_out, norm_out, norm_acc, norm_own, norm_all, norm_sems, cot, w1, w2, u_own, u_far, x_buf, d_act, hid, dh, part, got1, got2, gram_a, gram_b, sems, w_sems, u_sems, cot_sems, load_sems, dh_sems, dx_sems, all_sems, part_sems):
    n_layers, _, n_ex, seq, d_ff = u.shape
    d_model = x.shape[-1]
    pieces = cot.shape[1:]
    groups = n_ex // U_GROUP
    total = n_layers * n_ex
    summed = total - n_ex
    pos = place()
    core, partner = pos[0], pos[5]
    me = lax.axis_index("tp")
    others = [lax.rem(me + d, 8) for d in range(1, 8)]
    enter(others)
    ex = Exchange(pos, part, cot, got1, got2, sems, n_ex, 4)

    def layer_of(k):
        return n_layers - 1 - lax.div(k, n_ex)

    def weight_copies(layer):
        near = [
            pltpu.make_async_copy(w_down.at[layer], w2.at[layer, pl.ds(0, d_ff)], w_sems.at[0, layer, 0]),
            pltpu.make_async_copy(w_up.at[layer], w1.at[layer, :, pl.ds(0, d_ff)], w_sems.at[0, layer, 1]),
        ]
        far = [
            push(w_down.at[layer], w2.at[layer, pl.ds(d_ff, d_ff)], w_sems.at[1, layer, 0], w_sems.at[2, layer, 0], partner),
            push(w_up.at[layer], w1.at[layer, :, pl.ds(d_ff, d_ff)], w_sems.at[1, layer, 1], w_sems.at[2, layer, 1], partner),
        ]
        return near, far

    def far_copy(g):
        first = lax.rem(g, groups) * U_GROUP
        layer = n_layers - 1 - lax.div(g, groups)
        return push(u.at[layer, 1 - core, pl.ds(first, U_GROUP)], u_far.at[pl.ds(g * U_GROUP, U_GROUP)], u_sems.at[0, g], u_sems.at[1, g], partner)

    def cot_copy(e):
        return pltpu.make_async_copy(d_out.at[core, e], cot.at[e], cot_sems.at[e])

    def load_copies(p):
        k, s = example_at(p), lax.rem(p, 2)
        layer, e = layer_of(k), lax.rem(k, n_ex)
        return [
            pltpu.make_async_copy(u.at[layer, core, e], u_own.at[s], load_sems.at[s, 0]),
            pltpu.make_async_copy(x.at[layer, core, e], x_buf.at[s], load_sems.at[s, 1]),
        ]

    def dh_copies(p):
        k, s = example_at(p), lax.rem(p, 2)
        layer, e = layer_of(k), lax.rem(k, n_ex)
        near = pltpu.make_async_copy(dh.at[s, :, pl.ds(0, d_ff)], dh_out.at[layer, core, e], dh_sems.at[s, 0])
        far = push(dh.at[s, :, pl.ds(d_ff, d_ff)], dh_out.at[layer, core, e], dh_sems.at[s, 1], all_sems.at[0], partner)
        return near, far

    def dx_copies(j):
        step, e, s = lax.div(j, n_ex), lax.rem(j, n_ex), lax.rem(j, 4)
        near = pltpu.make_async_copy(cot.at[e], dx_out.at[step, core, e], dx_sems.at[s, 0])
        far = push(cot.at[e], dx_out.at[step, core, e], dx_sems.at[s, 1], all_sems.at[1], partner)
        return near, far

    def part_copy(k):
        s = lax.rem(k, 2)
        return pltpu.make_async_copy(part.at[4 + s], part_out.at[lax.rem(k, n_ex)], part_sems.at[s])

    early = summed - n_ex + 4 * LAG + 1

    def first_of(i):
        return jnp.where(i <= early, i, jnp.where(i < summed, 2 * i - early, i + summed - early))

    def example_at(p):
        r = p - early
        half = lax.div(r, 2)
        mixed = jnp.where(lax.rem(r, 2) == 0, early + half, summed + half)
        return jnp.where(jnp.logical_or(r < 0, p >= 2 * summed - early), p, mixed)

    def save(j):
        for copy in dx_copies(j):
            copy.start()

    def saved(j):
        near, far = dx_copies(j)
        near.wait()
        far.wait_send()

    top = n_layers - 1
    near, far = weight_copies(top)
    near[0].start()
    far[0].start()
    far_copy(0).start()
    cot_copy(0).start()
    for copy in load_copies(0):
        copy.start()
    near[1].start()
    far[1].start()

    @pl.loop(1, n_ex)
    def _(e):
        cot_copy(e).start()

    for layer in reversed(range(top)):
        for copy in sum(weight_copies(layer), []):
            copy.start()

    @pl.loop(1, n_layers * groups)
    def _(g):
        far_copy(g).start()

    norm_acc[...] = jnp.zeros_like(norm_acc)
    norm_own[...] = jnp.zeros_like(norm_own)

    def compute(p):
        k, s = example_at(p), lax.rem(p, 2)
        layer, e = layer_of(k), lax.rem(k, n_ex)

        @pl.when(lax.rem(k, n_ex) == 0)
        def _():
            near, far = weight_copies(layer)
            for copy in near:
                copy.wait()
            for copy in far:
                copy.wait_recv()

        @pl.when(lax.rem(k, U_GROUP) == 0)
        def _():
            far_copy(lax.div(k, U_GROUP)).wait_recv()

        @pl.when(k < n_ex)
        def _():
            cot_copy(e).wait()

        for copy in load_copies(p):
            copy.wait()

        @pl.when(p + 1 < total)
        def _():
            for copy in load_copies(p + 1):
                copy.start()

        @pl.when(p >= 2)
        def _():
            near, far = dh_copies(p - 2)
            near.wait()
            far.wait_send()

        @pl.when(k >= summed + 2)
        def _():
            part_copy(k - 2).wait()

        d_act[...] = lax.dot_general(cot[e].reshape(seq, d_model), w2[layer], NT, preferred_element_type=F32)
        rows = 32

        @pl.loop(0, seq // rows)
        def _(r):
            at = pl.ds(pl.multiple_of(r * rows, rows), rows)
            for half in range(2):
                columns = pl.ds(half * d_ff, d_ff)
                v = (u_own[s, at] if half == 0 else u_far[k, at]).astype(F32)
                square = v * v
                t = jnp.tanh(COEF * (v + CUBE * (square * v)))
                gate = 0.5 * (1.0 + t)
                slope = gate + (0.5 * v) * (1.0 - t * t) * (COEF * (1.0 + (3.0 * CUBE) * square))
                hid[at, columns] = (v * gate).astype(BF16)
                dh[s, at, columns] = (slope * d_act[at, columns]).astype(BF16)

        for copy in dh_copies(p):
            copy.start()
        back = lax.dot_general(dh[s], w1[layer], NT, preferred_element_type=F32)
        part[jnp.where(k < summed, lax.rem(k, 4), 4 + lax.rem(k, 2))] = back.astype(BF16).reshape(pieces)

        @pl.when(k < summed)
        def _():
            ex.start(0, k)

        @pl.when(k >= summed)
        def _():
            part_copy(k).start()

        for left, right in ((hid[...], cot[e].reshape(seq, d_model)), (x_buf[s], dh[s])):
            gram_a[...] = lax.dot_general(left, left, NT, preferred_element_type=F32)
            gram_b[...] = lax.dot_general(right, right, NT, preferred_element_type=F32)
            norm_acc[e] += jnp.sum((gram_a[...] * gram_b[...]).reshape(seq // 8, 8, seq), axis=0)

    @pl.loop(0, summed + 5 * LAG)
    def _(i):
        run_stages(ex, i, summed, save, saved)

        @pl.loop(first_of(i), first_of(i + 1))
        def _(p):
            compute(p)

    norm_own[0:n_ex] = jnp.sum(norm_acc[...], axis=1)
    for peer in others:
        push(norm_own, norm_all.at[me], norm_sems.at[0, peer], norm_sems.at[1, me], peer).start()
    norm_all[me] = norm_own[...]

    for k in (total - 2, total - 1):
        part_copy(k).wait()
    for k in (total - 2, total - 1):
        near, far = dh_copies(k)
        near.wait()
        far.wait_send()
    for peer in others:
        push(norm_own, norm_all.at[peer], norm_sems.at[0, peer], norm_sems.at[1, peer], peer).wait()
    for m in range(2):
        norm_out[m] = norm_all[m] + norm_all[m + 2] + norm_all[m + 4] + norm_all[m + 6]
    pltpu.make_async_copy(dh_out.at[:, 1 - core], dh_out.at[:, 1 - core], all_sems.at[0]).wait()
    pltpu.make_async_copy(dx_out.at[:, 1 - core], dx_out.at[:, 1 - core], all_sems.at[1]).wait()
    for layer in range(n_layers):
        for copy in weight_copies(layer)[1]:
            copy.wait_send()

    @pl.loop(0, n_layers * groups)
    def _(g):
        far_copy(g).wait_send()


def backward_call(u, x, w_up, w_down, d_out):
    n_layers, _, n_ex, seq, d_ff = u.shape
    d_model = x.shape[-1]
    pieces = (8, seq // 8, d_model)
    total = n_layers * n_ex
    rows = total * seq
    dma = pltpu.SemaphoreType.DMA
    return pl.pallas_call(
        backward_kernel,
        out_shape=(
            jax.ShapeDtypeStruct((n_layers - 1, 2, n_ex) + pieces, BF16),
            jax.ShapeDtypeStruct((n_layers, 2, n_ex, seq, d_ff), BF16),
            jax.ShapeDtypeStruct((n_ex,) + pieces, BF16),
            jax.ShapeDtypeStruct((2, 16, seq), F32),
        ),
        in_specs=[ANY] * 5,
        out_specs=(ANY, ANY, ANY, VMEM),
        scratch_shapes=[
            pltpu.VMEM((n_ex, 8, seq), F32),
            pltpu.VMEM((16, seq), F32),
            pltpu.VMEM((8, 16, seq), F32),
            dma((2, 8)),
            pltpu.VMEM((n_ex,) + pieces, BF16),
            pltpu.VMEM((n_layers, d_model, 2 * d_ff), BF16),
            pltpu.VMEM((n_layers, 2 * d_ff, d_model), BF16),
            pltpu.VMEM((2, seq, d_ff), BF16),
            pltpu.VMEM((total, seq, d_ff), BF16),
            pltpu.VMEM((2, seq, d_model), BF16),
            pltpu.VMEM((seq, 2 * d_ff), F32),
            pltpu.VMEM((seq, 2 * d_ff), BF16),
            pltpu.VMEM((2, seq, 2 * d_ff), BF16),
            pltpu.VMEM((6,) + pieces, BF16),
            pltpu.VMEM((4, 2, 2) + pieces[1:], BF16),
            pltpu.VMEM((4, 2) + pieces[1:], BF16),
            pltpu.VMEM((seq, seq), F32),
            pltpu.VMEM((seq, seq), F32),
            dma((2, 4, 4, 2)),
            dma((3, n_layers, 2)),
            dma((2, total // U_GROUP)),
            dma((n_ex,)),
            dma((2, 2)),
            dma((2, 2)),
            dma((4, 2)),
            dma((2,)),
            dma((2,)),
        ],
        compiler_params=pltpu.CompilerParams(collective_id=0, has_side_effects=True, vmem_limit_bytes=66_000_000),
        cost_estimate=pl.CostEstimate(flops=rows * d_model * d_ff * 16, bytes_accessed=rows * d_model * 16, transcendentals=rows * d_ff * 2),
        name="backward",
    )(u, x, w_up, w_down, d_out.reshape((2, n_ex) + pieces))


def gelu(v):
    return v * (0.5 * (1.0 + jnp.tanh(COEF * (v + CUBE * (v * v * v)))))


class Ring:
    def __init__(self, size, sums, got, sems, out):
        z = lax.axis_index("dp")
        self.z, self.size = z, size
        self.peers = lax.rem(z + 1, size), lax.rem(z + size - 1, size)
        self.sums, self.got, self.sems, self.out = sums, got, sems, out

    def tile(self, step, way):
        if way == 0:
            return 2 * lax.rem(self.z + 2 * self.size - 1 - step, self.size)
        return 2 * lax.rem(self.z + 1 + step, self.size) + 1

    def copies(self, step, j):
        s = lax.rem(j, 4)
        block = self.sums.at[lax.rem(lax.div(j, 4), 3), lax.rem(j, 4)]
        return [
            pltpu.make_async_remote_copy(
                src_ref=block.at[self.tile(step, way)],
                dst_ref=self.got.at[step, s, way],
                send_sem=self.sems.at[0, step, s, way],
                recv_sem=self.sems.at[1, step, s, way],
                device_id={"dp": self.peers[way]},
                device_id_type=pl.DeviceIdType.MESH,
            )
            for way in range(2)
        ]

    def start(self, step, j):
        for copy in self.copies(step, j):
            copy.start()

    def add(self, step, j):
        for copy in self.copies(step, j):
            copy.wait()
        g, q, s = lax.div(j, 4), lax.rem(j, 4), lax.rem(j, 4)
        for way in range(2):
            at = lax.rem(g, 3), q, self.tile(step + 1, way)
            total = self.sums[at] + self.got[step, s, way]
            if step + 1 < self.size - 1:
                self.sums[at] = total
            else:
                rows, columns = total.shape
                self.out[g, pl.ds(pl.multiple_of(q * rows, rows), rows), pl.ds(way * columns, columns)] = total
        if step + 1 < self.size - 1:
            self.start(step + 1, j)


def gradient_kernel(size, part_in, dx_in, d_out, x, dh, u, clip, d_in, grads, cot, part, got1, got2, sums, got_z, a_buf, b_buf, a_scaled, b_scaled, sems, in_sems, dx_sems, all_sems, z_sems, load_sems):
    n_layers, _, n_ex, seq, d_ff = u.shape
    d_model = x.shape[-1]
    pairs = n_ex // 2
    per_grad = 2 * pairs
    per_step = per_grad // 4
    n_grads = 2 * n_layers
    steps = n_grads * per_grad
    last = n_layers - 2
    pos = place()
    core, partner = pos[0], pos[5]
    ring = Ring(size, sums, got_z, z_sems, grads)
    barrier = pltpu.get_barrier_semaphore()
    for peer in pos[3:]:
        pl.semaphore_signal(barrier, inc=1, device_id={"tp": peer}, device_id_type=pl.DeviceIdType.MESH)
    if size > 1:
        for peer in ring.peers:
            pl.semaphore_signal(barrier, inc=1, device_id={"dp": peer}, device_id_type=pl.DeviceIdType.MESH)
    pl.semaphore_wait(barrier, 5 if size > 1 else 3)
    ex = Exchange(pos, part, cot, got1, got2, sems, n_ex, n_ex)

    def in_copies(e):
        return [
            pltpu.make_async_copy(part_in.at[e], part.at[e], in_sems.at[e, 0]),
            pltpu.make_async_copy(dx_in.at[last, core, e], cot.at[e], in_sems.at[e, 1]),
        ]

    def dx_copies(j):
        s = lax.rem(j, 4)
        near = pltpu.make_async_copy(cot.at[j], d_in.at[core, j], dx_sems.at[s, 0])
        far = push(cot.at[j], d_in.at[core, j], dx_sems.at[s, 1], all_sems.at[0], partner)
        return near, far

    def save(j):
        for copy in dx_copies(j):
            copy.start()

    def saved(j):
        near, far = dx_copies(j)
        near.wait()
        far.wait_send()

    def where_is(t):
        g, pair = lax.div(t, per_grad), lax.rem(t, per_grad)
        return g, lax.rem(g, n_layers), lax.div(pair, pairs), 2 * lax.rem(pair, pairs), lax.rem(t, 2)

    def load(t):
        g, layer, m, e, s = where_is(t)
        two = pl.ds(e, 2)

        @pl.when(g < n_layers)
        def _():
            pltpu.make_async_copy(x.at[layer, m, two], a_buf.at[s], load_sems.at[s, 0]).start()
            pltpu.make_async_copy(dh.at[layer, m, two], b_buf.at[s], load_sems.at[s, 1]).start()

        @pl.when(g >= n_layers)
        def _():
            pltpu.make_async_copy(u.at[layer, m, two], b_buf.at[s], load_sems.at[s, 1]).start()

        @pl.when(g == n_grads - 1)
        def _():
            pltpu.make_async_copy(d_out.at[m, two], a_buf.at[s], load_sems.at[s, 0]).start()

        @pl.when(jnp.logical_and(g >= n_layers, g < n_grads - 1))
        def _():
            pltpu.make_async_copy(dx_in.at[last - layer, m, two], a_buf.at[s], load_sems.at[s, 0]).start()

    def accumulate(t):
        g, layer, m, e, s = where_is(t)

        @pl.when(t + 1 < steps)
        def _():
            load(t + 1)

        pltpu.make_async_copy(x.at[0, 0, pl.ds(0, 2)], a_buf.at[s], load_sems.at[s, 0]).wait()
        pltpu.make_async_copy(u.at[0, 0, pl.ds(0, 2)], b_buf.at[s], load_sems.at[s, 1]).wait()
        slot = lax.rem(g, 3)

        def add(b, a):
            c = lax.dot_general(b, a, (((0,), (0,)), ((), ())), preferred_element_type=F32)
            tiles, _, rows, columns = sums.shape[1:]
            first = lax.rem(t, per_grad) == 0
            for n in range(2 * size):
                new = c[:, n * columns:(n + 1) * columns].reshape(tiles, rows, columns)
                old = jnp.where(first, 0.0, sums[slot, :, n])
                sums[slot, :, n] = old + new

        @pl.when(g < n_layers)
        def _():
            for i in range(2):
                b_scaled[i * seq:(i + 1) * seq] = (b_buf[s, i].astype(F32) * clip[m * n_ex + e + i]).astype(BF16)
            add(b_scaled[...], a_buf[s].reshape(2 * seq, d_model))

        @pl.when(g >= n_layers)
        def _():
            for i in range(2):
                a_scaled[i * seq:(i + 1) * seq] = (a_buf[s, i].reshape(seq, d_model).astype(F32) * clip[m * n_ex + e + i]).astype(BF16)
                b_scaled[i * seq:(i + 1) * seq] = gelu(b_buf[s, i].astype(F32)).astype(BF16)
            add(b_scaled[...], a_scaled[...])

    load(0)

    @pl.loop(0, n_ex)
    def _(e):
        for copy in in_copies(e):
            copy.start()

    blocks = 4 * n_grads

    @pl.loop(0, max(blocks + 4 + size - 1, 2 * (n_ex + 5 * LAG)))
    def _(i):
        j = i - 4
        for step in (0, *reversed(range(1, size))):
            @pl.when(jnp.logical_and(j - step >= 0, j - step < blocks))
            def _(step=step):
                if step == 0:
                    ring.start(0, j)
                else:
                    ring.add(step - 1, j - step)

        @pl.when(lax.rem(i, 2) == 0)
        def _():
            k = lax.div(i, 2)

            @pl.when(k < n_ex)
            def _():
                for copy in in_copies(k):
                    copy.wait()
                ex.start(0, k)

            run_stages(ex, k, n_ex, save, saved)

        @pl.when(i < blocks)
        def _():
            @pl.loop(0, per_step)
            def _(r):
                accumulate(i * per_step + r)

    pltpu.make_async_copy(d_in.at[1 - core], d_in.at[1 - core], all_sems.at[0]).wait()


def gradient_call(size, part, dx, d_out, x, dh, u, clip):
    n_layers, _, n_ex, seq, d_ff = u.shape
    d_model = x.shape[-1]
    pieces = part.shape[1:]
    width = d_model // (2 * size)
    dma = pltpu.SemaphoreType.DMA
    return pl.pallas_call(
        functools.partial(gradient_kernel, size),
        out_shape=(
            jax.ShapeDtypeStruct((2, n_ex) + pieces, BF16),
            jax.ShapeDtypeStruct((2 * n_layers, d_ff, 2 * width), F32),
        ),
        in_specs=[ANY] * 6 + [pl.BlockSpec(memory_space=pltpu.SMEM)],
        out_specs=(ANY, VMEM),
        scratch_shapes=[
            pltpu.VMEM((n_ex,) + pieces, BF16),
            pltpu.VMEM((n_ex,) + pieces, BF16),
            pltpu.VMEM((4, 2, 2) + pieces[1:], BF16),
            pltpu.VMEM((4, 2) + pieces[1:], BF16),
            pltpu.VMEM((3, 4, 2 * size, d_ff // 4, width), F32),
            pltpu.VMEM((size - 1, 4, 2, d_ff // 4, width), F32),
            pltpu.VMEM((2, 2) + pieces, BF16),
            pltpu.VMEM((2, 2, seq, d_ff), BF16),
            pltpu.VMEM((2 * seq, d_model), BF16),
            pltpu.VMEM((2 * seq, d_ff), BF16),
            dma((2, 4, 4, 2)),
            dma((n_ex, 2)),
            dma((4, 2)),
            dma((1,)),
            dma((2, size - 1, 4, 2)),
            dma((2, 2)),
        ],
        compiler_params=pltpu.CompilerParams(collective_id=1, has_side_effects=True, vmem_limit_bytes=66_000_000),
        name="gradient",
    )(part, dx, d_out.reshape((2, n_ex) + pieces), x.reshape((n_layers, 2, n_ex) + pieces), dh, u, clip)


def finish_kernel(examples, n_layers, d_in, up_sum, down_sum, noise_up, noise_down, clip_norm, noise_mult, up_grad, down_grad, d_in_out):
    i = pl.program_id(0)
    d_in_out[...] = d_in[...]
    noise_scale = noise_mult[0] * clip_norm[0]

    @pl.when(i < n_layers)
    def _():
        up_grad[0] = (up_sum[0].T + noise_scale * noise_up[0]) / examples

    @pl.when(i >= n_layers)
    def _():
        down_grad[0] = (down_sum[0] + noise_scale * noise_down[0]) / examples


def finish_call(examples, d_in, sums, noise_up, noise_down, clip_norm, noise_mult):
    n_layers, width, d_ff = noise_up.shape
    rows, seq, d_model = d_in.shape
    steps = 2 * n_layers

    def early(i):
        return jnp.minimum(i, n_layers - 1), 0, 0

    def late(i):
        return jnp.maximum(i - n_layers, 0), 0, 0

    def late_sum(i):
        return jnp.maximum(i, n_layers), 0, 0

    def same(i):
        return i, 0, 0

    smem = pl.BlockSpec(memory_space=pltpu.SMEM)
    block = pl.BlockSpec((rows // steps, seq, d_model), same)
    return pl.pallas_call(
        functools.partial(finish_kernel, examples, n_layers),
        grid=(steps,),
        out_shape=(
            jax.ShapeDtypeStruct((n_layers, width, d_ff), F32),
            jax.ShapeDtypeStruct((n_layers, d_ff, width), F32),
            jax.ShapeDtypeStruct(d_in.shape, BF16),
        ),
        in_specs=[
            block,
            pl.BlockSpec((1, d_ff, width), early),
            pl.BlockSpec((1, d_ff, width), late_sum),
            pl.BlockSpec((1, width, d_ff), early),
            pl.BlockSpec((1, d_ff, width), late),
            smem,
            smem,
        ],
        out_specs=(pl.BlockSpec((1, width, d_ff), early), pl.BlockSpec((1, d_ff, width), late), block),
        compiler_params=pltpu.CompilerParams(vmem_limit_bytes=66_000_000),
        name="finish",
    )(d_in, sums, sums, noise_up, noise_down, clip_norm, noise_mult)


def solution(mesh):
    dp_size = mesh.shape["dp"]

    def local_pass(x_in, u_pre, w_up, w_down, d_out, noise_up, noise_down, clip_norm, noise_mult):
        examples = d_out.shape[0] * d_out.shape[1] * dp_size
        dx, dh, part, norms = backward_call(u_pre, x_in, w_up, w_down, d_out)
        norm_vec = jnp.sum(norms, axis=2)[:, :d_out.shape[1]]
        clip_fac = jnp.minimum(1.0, clip_norm[0] / jnp.sqrt(norm_vec)).reshape(-1)
        d_in, sums = gradient_call(dp_size, part, dx, d_out, x_in, dh, u_pre, clip_fac)
        d_in = d_in.reshape((-1,) + d_out.shape[2:])
        up_grad, down_grad, d_in = finish_call(examples, d_in, sums, noise_up, noise_down, clip_norm, noise_mult)
        return up_grad, down_grad, d_in.reshape(d_out.shape)

    in_specs = (P(None, None, "dp", None, None), P(None, None, "dp", None, "tp"), P(None, None, "tp"), P(None, "tp", None), P(None, "dp", None, None), P(None, "dp", "tp"), P(None, "tp", "dp"), P(), P())
    out_specs = (P(None, "dp", "tp"), P(None, "tp", "dp"), P(None, "dp", None, None))
    return jax.shard_map(local_pass, mesh=mesh, in_specs=in_specs, out_specs=out_specs, check_vma=False)
```

```python
import functools
import math

import jax
import jax.numpy as jnp
from jax import lax
from jax.experimental import pallas as pl
from jax.experimental.pallas import tpu as pltpu
from jax.sharding import PartitionSpec as P

F32 = jnp.float32
BF16 = jnp.bfloat16
NT = (((1,), (1,)), ((), ()))
ANY = pl.BlockSpec(memory_space=pl.ANY)
VMEM = pl.BlockSpec(memory_space=pltpu.VMEM)
LAG = 1
U_GROUP = 2
COEF = math.sqrt(2.0 / math.pi)
CUBE = 0.044715


def place():
    t = lax.axis_index("tp")
    core = lax.rem(t, 2)
    px = lax.rem(lax.div(t, 2), 2)
    py = lax.div(t, 4)
    return core, px, py, t + 2 - 4 * px, t + 4 - 8 * py, t + 1 - 2 * core


def enter(peers):
    barrier = pltpu.get_barrier_semaphore()
    for peer in peers:
        pl.semaphore_signal(barrier, inc=1, device_id={"tp": peer}, device_id_type=pl.DeviceIdType.MESH)
    pl.semaphore_wait(barrier, len(peers))


def push(src, dst, send_sem, recv_sem, peer):
    return pltpu.make_async_remote_copy(src_ref=src, dst_ref=dst, send_sem=send_sem, recv_sem=recv_sem, device_id={"tp": peer}, device_id_type=pl.DeviceIdType.MESH)


class Exchange:
    def __init__(self, pos, part, cot, got1, got2, sems, n_examples, n_slots):
        self.core, self.px, self.py, self.nx, self.ny, self.partner = pos
        self.part, self.cot, self.got1, self.got2, self.sems = part, cot, got1, got2, sems
        self.n_examples, self.n_slots = n_examples, n_slots

    def copies(self, kind, j):
        px, py = self.px, self.py
        part = self.part.at[lax.rem(j, self.n_slots)]
        cot = self.cot.at[lax.rem(j, self.n_examples)]
        s = lax.rem(j, 4)
        send, recv = self.sems.at[0, kind], self.sems.at[1, kind]
        if kind == 0:
            pairs = ((part.at[pl.ds(2 * (1 - px), 2)], self.got1.at[s, 0], self.nx), (part.at[pl.ds(4 + 2 * (1 - py), 2)], self.got1.at[s, 1], self.ny))
        elif kind == 1:
            pairs = ((part.at[2 * px + 1 - py], self.got2.at[s, 0], self.ny), (part.at[4 + 2 * py + 1 - px], self.got2.at[s, 1], self.nx))
        elif kind == 2:
            own_a, own_b = cot.at[2 * px + py], cot.at[4 + 2 * py + px]
            pairs = ((own_a, own_a, self.ny), (own_b, own_b, self.nx))
        else:
            two_a, two_b = cot.at[pl.ds(2 * px, 2)], cot.at[pl.ds(4 + 2 * py, 2)]
            pairs = ((two_a, two_a, self.nx), (two_b, two_b, self.ny))
        return [push(src, dst, send.at[s, c], recv.at[s, c], peer) for c, (src, dst, peer) in enumerate(pairs)]

    def start(self, kind, j):
        for copy in self.copies(kind, j):
            copy.start()

    def wait(self, kind, j):
        for copy in self.copies(kind, j):
            copy.wait()

    def add_first(self, j):
        self.wait(0, j)
        slot, s = lax.rem(j, self.n_slots), lax.rem(j, 4)
        for c, first in enumerate((2 * self.px, 4 + 2 * self.py)):
            for i in range(2):
                mine = self.part[slot, first + i].astype(F32) + self.got1[s, c, i].astype(F32)
                self.part[slot, first + i] = mine.astype(BF16)
        self.start(1, j)

    def add_second(self, j):
        self.wait(1, j)
        slot, s, e = lax.rem(j, self.n_slots), lax.rem(j, 4), lax.rem(j, self.n_examples)
        for c, own in enumerate((2 * self.px + self.py, 4 + 2 * self.py + self.px)):
            back = self.part[slot, own].astype(F32) + self.got2[s, c].astype(F32)
            self.cot[e, own] = (self.cot[e, own].astype(F32) + back).astype(BF16)
        self.start(2, j)

    def forward(self, j):
        self.wait(2, j)
        self.start(3, j)


def run_stages(ex, k, count, save, saved):
    def at(lag, fn):
        j = k - lag * LAG

        @pl.when(jnp.logical_and(j >= 0, j < count))
        def _():
            fn(j)

    def finish(j):
        ex.wait(3, j)
        save(j)

    at(5, saved)
    at(4, finish)
    at(3, ex.forward)
    at(2, ex.add_second)
    at(1, ex.add_first)


def backward_kernel(u, x, w_up, w_down, d_out, dx_out, dh_out, part_out, norm_out, norm_acc, norm_own, norm_all, norm_sems, cot, w1, w2, u_own, u_far, x_buf, d_act, hid, dh, part, got1, got2, gram_a, gram_b, sems, w_sems, u_sems, cot_sems, load_sems, dh_sems, dx_sems, all_sems, part_sems):
    n_layers, _, n_ex, seq, d_ff = u.shape
    d_model = x.shape[-1]
    pieces = cot.shape[1:]
    groups = n_ex // U_GROUP
    total = n_layers * n_ex
    summed = total - n_ex
    pos = place()
    core, partner = pos[0], pos[5]
    me = lax.axis_index("tp")
    others = [lax.rem(me + d, 8) for d in range(1, 8)]
    enter(others)
    ex = Exchange(pos, part, cot, got1, got2, sems, n_ex, 4)

    def layer_of(k):
        return n_layers - 1 - lax.div(k, n_ex)

    def weight_copies(layer):
        near = [
            pltpu.make_async_copy(w_down.at[layer], w2.at[layer, pl.ds(0, d_ff)], w_sems.at[0, layer, 0]),
            pltpu.make_async_copy(w_up.at[layer], w1.at[layer, :, pl.ds(0, d_ff)], w_sems.at[0, layer, 1]),
        ]
        far = [
            push(w_down.at[layer], w2.at[layer, pl.ds(d_ff, d_ff)], w_sems.at[1, layer, 0], w_sems.at[2, layer, 0], partner),
            push(w_up.at[layer], w1.at[layer, :, pl.ds(d_ff, d_ff)], w_sems.at[1, layer, 1], w_sems.at[2, layer, 1], partner),
        ]
        return near, far

    def far_copy(g):
        first = lax.rem(g, groups) * U_GROUP
        layer = n_layers - 1 - lax.div(g, groups)
        return push(u.at[layer, 1 - core, pl.ds(first, U_GROUP)], u_far.at[pl.ds(g * U_GROUP, U_GROUP)], u_sems.at[0, g], u_sems.at[1, g], partner)

    def cot_copy(e):
        return pltpu.make_async_copy(d_out.at[core, e], cot.at[e], cot_sems.at[e])

    def load_copies(p):
        k, s = example_at(p), lax.rem(p, 2)
        layer, e = layer_of(k), lax.rem(k, n_ex)
        return [
            pltpu.make_async_copy(u.at[layer, core, e], u_own.at[s], load_sems.at[s, 0]),
            pltpu.make_async_copy(x.at[layer, core, e], x_buf.at[s], load_sems.at[s, 1]),
        ]

    def dh_copies(p):
        k, s = example_at(p), lax.rem(p, 2)
        layer, e = layer_of(k), lax.rem(k, n_ex)
        near = pltpu.make_async_copy(dh.at[s, :, pl.ds(0, d_ff)], dh_out.at[layer, core, e], dh_sems.at[s, 0])
        far = push(dh.at[s, :, pl.ds(d_ff, d_ff)], dh_out.at[layer, core, e], dh_sems.at[s, 1], all_sems.at[0], partner)
        return near, far

    def dx_copies(j):
        step, e, s = lax.div(j, n_ex), lax.rem(j, n_ex), lax.rem(j, 4)
        near = pltpu.make_async_copy(cot.at[e], dx_out.at[step, core, e], dx_sems.at[s, 0])
        far = push(cot.at[e], dx_out.at[step, core, e], dx_sems.at[s, 1], all_sems.at[1], partner)
        return near, far

    def part_copy(k):
        s = lax.rem(k, 2)
        return pltpu.make_async_copy(part.at[4 + s], part_out.at[lax.rem(k, n_ex)], part_sems.at[s])

    early = summed - n_ex + 4 * LAG + 1

    def first_of(i):
        return jnp.where(i <= early, i, jnp.where(i < summed, 2 * i - early, i + summed - early))

    def example_at(p):
        r = p - early
        half = lax.div(r, 2)
        mixed = jnp.where(lax.rem(r, 2) == 0, early + half, summed + half)
        return jnp.where(jnp.logical_or(r < 0, p >= 2 * summed - early), p, mixed)

    def save(j):
        for copy in dx_copies(j):
            copy.start()

    def saved(j):
        near, far = dx_copies(j)
        near.wait()
        far.wait_send()

    top = n_layers - 1
    near, far = weight_copies(top)
    near[0].start()
    far[0].start()
    far_copy(0).start()
    cot_copy(0).start()
    for copy in load_copies(0):
        copy.start()
    near[1].start()
    far[1].start()

    @pl.loop(1, n_ex)
    def _(e):
        cot_copy(e).start()

    for layer in reversed(range(top)):
        for copy in sum(weight_copies(layer), []):
            copy.start()

    @pl.loop(1, n_layers * groups)
    def _(g):
        far_copy(g).start()

    norm_acc[...] = jnp.zeros_like(norm_acc)
    norm_own[...] = jnp.zeros_like(norm_own)

    def compute(p):
        k, s = example_at(p), lax.rem(p, 2)
        layer, e = layer_of(k), lax.rem(k, n_ex)

        @pl.when(lax.rem(k, n_ex) == 0)
        def _():
            near, far = weight_copies(layer)
            for copy in near:
                copy.wait()
            for copy in far:
                copy.wait_recv()

        @pl.when(lax.rem(k, U_GROUP) == 0)
        def _():
            far_copy(lax.div(k, U_GROUP)).wait_recv()

        @pl.when(k < n_ex)
        def _():
            cot_copy(e).wait()

        for copy in load_copies(p):
            copy.wait()

        @pl.when(p + 1 < total)
        def _():
            for copy in load_copies(p + 1):
                copy.start()

        @pl.when(p >= 2)
        def _():
            near, far = dh_copies(p - 2)
            near.wait()
            far.wait_send()

        @pl.when(k >= summed + 2)
        def _():
            part_copy(k - 2).wait()

        d_act[...] = lax.dot_general(cot[e].reshape(seq, d_model), w2[layer], NT, preferred_element_type=F32)
        rows = 32

        @pl.loop(0, seq // rows)
        def _(r):
            at = pl.ds(pl.multiple_of(r * rows, rows), rows)
            for half in range(2):
                columns = pl.ds(half * d_ff, d_ff)
                v = (u_own[s, at] if half == 0 else u_far[k, at]).astype(F32)
                square = v * v
                t = jnp.tanh(COEF * (v + CUBE * (square * v)))
                gate = 0.5 * (1.0 + t)
                slope = gate + (0.5 * v) * (1.0 - t * t) * (COEF * (1.0 + (3.0 * CUBE) * square))
                hid[at, columns] = (v * gate).astype(BF16)
                dh[s, at, columns] = (slope * d_act[at, columns]).astype(BF16)

        for copy in dh_copies(p):
            copy.start()
        back = lax.dot_general(dh[s], w1[layer], NT, preferred_element_type=F32)
        part[jnp.where(k < summed, lax.rem(k, 4), 4 + lax.rem(k, 2))] = back.astype(BF16).reshape(pieces)

        @pl.when(k < summed)
        def _():
            ex.start(0, k)

        @pl.when(k >= summed)
        def _():
            part_copy(k).start()

        for left, right in ((hid[...], cot[e].reshape(seq, d_model)), (x_buf[s], dh[s])):
            gram_a[...] = lax.dot_general(left, left, NT, preferred_element_type=F32)
            gram_b[...] = lax.dot_general(right, right, NT, preferred_element_type=F32)
            norm_acc[e] += jnp.sum((gram_a[...] * gram_b[...]).reshape(seq // 8, 8, seq), axis=0)

    @pl.loop(0, summed + 5 * LAG)
    def _(i):
        run_stages(ex, i, summed, save, saved)

        @pl.loop(first_of(i), first_of(i + 1))
        def _(p):
            compute(p)

    norm_own[0:n_ex] = jnp.sum(norm_acc[...], axis=1)
    for peer in others:
        push(norm_own, norm_all.at[me], norm_sems.at[0, peer], norm_sems.at[1, me], peer).start()
    norm_all[me] = norm_own[...]

    for k in (total - 2, total - 1):
        part_copy(k).wait()
    for k in (total - 2, total - 1):
        near, far = dh_copies(k)
        near.wait()
        far.wait_send()
    for peer in others:
        push(norm_own, norm_all.at[peer], norm_sems.at[0, peer], norm_sems.at[1, peer], peer).wait()
    for m in range(2):
        norm_out[m] = norm_all[m] + norm_all[m + 2] + norm_all[m + 4] + norm_all[m + 6]
    pltpu.make_async_copy(dh_out.at[:, 1 - core], dh_out.at[:, 1 - core], all_sems.at[0]).wait()
    pltpu.make_async_copy(dx_out.at[:, 1 - core], dx_out.at[:, 1 - core], all_sems.at[1]).wait()
    for layer in range(n_layers):
        for copy in weight_copies(layer)[1]:
            copy.wait_send()

    @pl.loop(0, n_layers * groups)
    def _(g):
        far_copy(g).wait_send()


def backward_call(u, x, w_up, w_down, d_out):
    n_layers, _, n_ex, seq, d_ff = u.shape
    d_model = x.shape[-1]
    pieces = (8, seq // 8, d_model)
    total = n_layers * n_ex
    rows = total * seq
    dma = pltpu.SemaphoreType.DMA
    return pl.pallas_call(
        backward_kernel,
        out_shape=(
            jax.ShapeDtypeStruct((n_layers - 1, 2, n_ex) + pieces, BF16),
            jax.ShapeDtypeStruct((n_layers, 2, n_ex, seq, d_ff), BF16),
            jax.ShapeDtypeStruct((n_ex,) + pieces, BF16),
            jax.ShapeDtypeStruct((2, 16, seq), F32),
        ),
        in_specs=[ANY] * 5,
        out_specs=(ANY, ANY, ANY, VMEM),
        scratch_shapes=[
            pltpu.VMEM((n_ex, 8, seq), F32),
            pltpu.VMEM((16, seq), F32),
            pltpu.VMEM((8, 16, seq), F32),
            dma((2, 8)),
            pltpu.VMEM((n_ex,) + pieces, BF16),
            pltpu.VMEM((n_layers, d_model, 2 * d_ff), BF16),
            pltpu.VMEM((n_layers, 2 * d_ff, d_model), BF16),
            pltpu.VMEM((2, seq, d_ff), BF16),
            pltpu.VMEM((total, seq, d_ff), BF16),
            pltpu.VMEM((2, seq, d_model), BF16),
            pltpu.VMEM((seq, 2 * d_ff), F32),
            pltpu.VMEM((seq, 2 * d_ff), BF16),
            pltpu.VMEM((2, seq, 2 * d_ff), BF16),
            pltpu.VMEM((6,) + pieces, BF16),
            pltpu.VMEM((4, 2, 2) + pieces[1:], BF16),
            pltpu.VMEM((4, 2) + pieces[1:], BF16),
            pltpu.VMEM((seq, seq), F32),
            pltpu.VMEM((seq, seq), F32),
            dma((2, 4, 4, 2)),
            dma((3, n_layers, 2)),
            dma((2, total // U_GROUP)),
            dma((n_ex,)),
            dma((2, 2)),
            dma((2, 2)),
            dma((4, 2)),
            dma((2,)),
            dma((2,)),
        ],
        compiler_params=pltpu.CompilerParams(collective_id=0, has_side_effects=True, vmem_limit_bytes=66_000_000),
        cost_estimate=pl.CostEstimate(flops=rows * d_model * d_ff * 16, bytes_accessed=rows * d_model * 16, transcendentals=rows * d_ff * 2),
        name="backward",
    )(u, x, w_up, w_down, d_out.reshape((2, n_ex) + pieces))


def gelu(v):
    return v * (0.5 * (1.0 + jnp.tanh(COEF * (v + CUBE * (v * v * v)))))


class Ring:
    def __init__(self, size, sums, got, sems, out):
        z = lax.axis_index("dp")
        self.z, self.size = z, size
        self.peers = lax.rem(z + 1, size), lax.rem(z + size - 1, size)
        self.sums, self.got, self.sems, self.out = sums, got, sems, out

    def tile(self, step, way):
        if way == 0:
            return 2 * lax.rem(self.z + 2 * self.size - 1 - step, self.size)
        return 2 * lax.rem(self.z + 1 + step, self.size) + 1

    def copies(self, step, j):
        s = lax.rem(j, 8)
        block = self.sums.at[lax.rem(lax.div(j, 4), 4), lax.rem(j, 4)]
        return [
            pltpu.make_async_remote_copy(
                src_ref=block.at[self.tile(step, way)],
                dst_ref=self.got.at[step, s, way],
                send_sem=self.sems.at[0, step, s, way],
                recv_sem=self.sems.at[1, step, s, way],
                device_id={"dp": self.peers[way]},
                device_id_type=pl.DeviceIdType.MESH,
            )
            for way in range(2)
        ]

    def start(self, step, j):
        for copy in self.copies(step, j):
            copy.start()

    def add(self, step, j):
        for copy in self.copies(step, j):
            copy.wait()
        g, q, s = lax.div(j, 4), lax.rem(j, 4), lax.rem(j, 8)
        for way in range(2):
            at = lax.rem(g, 4), q, self.tile(step + 1, way)
            total = self.sums[at] + self.got[step, s, way]
            if step + 1 < self.size - 1:
                self.sums[at] = total
            else:
                rows, columns = total.shape
                self.out[g, pl.ds(pl.multiple_of(q * rows, rows), rows), pl.ds(way * columns, columns)] = total
        if step + 1 < self.size - 1:
            self.start(step + 1, j)


def gradient_kernel(size, part_in, dx_in, d_out, x, dh, u, clip, d_in, grads, cot, part, got1, got2, sums, got_z, a_buf, b_buf, a_scaled, b_scaled, sems, in_sems, dx_sems, all_sems, z_sems, load_sems):
    n_layers, _, n_ex, seq, d_ff = u.shape
    d_model = x.shape[-1]
    pairs = n_ex // 2
    per_grad = 2 * pairs
    per_step = per_grad // 4
    n_grads = 2 * n_layers
    steps = n_grads * per_grad
    last = n_layers - 2
    pos = place()
    core, partner = pos[0], pos[5]
    ring = Ring(size, sums, got_z, z_sems, grads)
    barrier = pltpu.get_barrier_semaphore()
    for peer in pos[3:]:
        pl.semaphore_signal(barrier, inc=1, device_id={"tp": peer}, device_id_type=pl.DeviceIdType.MESH)
    if size > 1:
        for peer in ring.peers:
            pl.semaphore_signal(barrier, inc=1, device_id={"dp": peer}, device_id_type=pl.DeviceIdType.MESH)
    pl.semaphore_wait(barrier, 5 if size > 1 else 3)
    ex = Exchange(pos, part, cot, got1, got2, sems, n_ex, n_ex)

    def in_copies(e):
        return [
            pltpu.make_async_copy(part_in.at[e], part.at[e], in_sems.at[e, 0]),
            pltpu.make_async_copy(dx_in.at[last, core, e], cot.at[e], in_sems.at[e, 1]),
        ]

    def dx_copies(j):
        s = lax.rem(j, 4)
        near = pltpu.make_async_copy(cot.at[j], d_in.at[core, j], dx_sems.at[s, 0])
        far = push(cot.at[j], d_in.at[core, j], dx_sems.at[s, 1], all_sems.at[0], partner)
        return near, far

    def save(j):
        for copy in dx_copies(j):
            copy.start()

    def saved(j):
        near, far = dx_copies(j)
        near.wait()
        far.wait_send()

    def where_is(t):
        g, pair = lax.div(t, per_grad), lax.rem(t, per_grad)
        return g, lax.rem(g, n_layers), lax.div(pair, pairs), 2 * lax.rem(pair, pairs), lax.rem(t, 2)

    def load(t):
        g, layer, m, e, s = where_is(t)
        two = pl.ds(e, 2)

        @pl.when(g < n_layers)
        def _():
            pltpu.make_async_copy(x.at[layer, m, two], a_buf.at[s], load_sems.at[s, 0]).start()
            pltpu.make_async_copy(dh.at[layer, m, two], b_buf.at[s], load_sems.at[s, 1]).start()

        @pl.when(g >= n_layers)
        def _():
            pltpu.make_async_copy(u.at[layer, m, two], b_buf.at[s], load_sems.at[s, 1]).start()

        @pl.when(g == n_grads - 1)
        def _():
            pltpu.make_async_copy(d_out.at[m, two], a_buf.at[s], load_sems.at[s, 0]).start()

        @pl.when(jnp.logical_and(g >= n_layers, g < n_grads - 1))
        def _():
            pltpu.make_async_copy(dx_in.at[last - layer, m, two], a_buf.at[s], load_sems.at[s, 0]).start()

    def accumulate(t):
        g, layer, m, e, s = where_is(t)

        @pl.when(t + 1 < steps)
        def _():
            load(t + 1)

        pltpu.make_async_copy(x.at[0, 0, pl.ds(0, 2)], a_buf.at[s], load_sems.at[s, 0]).wait()
        pltpu.make_async_copy(u.at[0, 0, pl.ds(0, 2)], b_buf.at[s], load_sems.at[s, 1]).wait()
        slot = lax.rem(g, 4)

        def add(b, a):
            c = lax.dot_general(b, a, (((0,), (0,)), ((), ())), preferred_element_type=F32)
            tiles, _, rows, columns = sums.shape[1:]
            first = lax.rem(t, per_grad) == 0
            for n in range(2 * size):
                new = c[:, n * columns:(n + 1) * columns].reshape(tiles, rows, columns)
                old = jnp.where(first, 0.0, sums[slot, :, n])
                sums[slot, :, n] = old + new

        @pl.when(g < n_layers)
        def _():
            for i in range(2):
                b_scaled[i * seq:(i + 1) * seq] = (b_buf[s, i].astype(F32) * clip[m * n_ex + e + i]).astype(BF16)
            add(b_scaled[...], a_buf[s].reshape(2 * seq, d_model))

        @pl.when(g >= n_layers)
        def _():
            for i in range(2):
                a_scaled[i * seq:(i + 1) * seq] = (a_buf[s, i].reshape(seq, d_model).astype(F32) * clip[m * n_ex + e + i]).astype(BF16)
                b_scaled[i * seq:(i + 1) * seq] = gelu(b_buf[s, i].astype(F32)).astype(BF16)
            add(b_scaled[...], a_scaled[...])

    load(0)

    @pl.loop(0, n_ex)
    def _(e):
        for copy in in_copies(e):
            copy.start()

    blocks = 4 * n_grads

    @pl.loop(0, max(blocks + 4 + 2 * (size - 1), 2 * (n_ex + 5 * LAG)))
    def _(i):
        j = i - 4
        for step in (0, *reversed(range(1, size))):
            @pl.when(jnp.logical_and(j - 2 * step >= 0, j - 2 * step < blocks))
            def _(step=step):
                if step == 0:
                    ring.start(0, j)
                else:
                    ring.add(step - 1, j - 2 * step)

        @pl.when(lax.rem(i, 2) == 0)
        def _():
            k = lax.div(i, 2)

            @pl.when(k < n_ex)
            def _():
                for copy in in_copies(k):
                    copy.wait()
                ex.start(0, k)

            run_stages(ex, k, n_ex, save, saved)

        @pl.when(i < blocks)
        def _():
            @pl.loop(0, per_step)
            def _(r):
                accumulate(i * per_step + r)

    pltpu.make_async_copy(d_in.at[1 - core], d_in.at[1 - core], all_sems.at[0]).wait()


def gradient_call(size, part, dx, d_out, x, dh, u, clip):
    n_layers, _, n_ex, seq, d_ff = u.shape
    d_model = x.shape[-1]
    pieces = part.shape[1:]
    width = d_model // (2 * size)
    dma = pltpu.SemaphoreType.DMA
    return pl.pallas_call(
        functools.partial(gradient_kernel, size),
        out_shape=(
            jax.ShapeDtypeStruct((2, n_ex) + pieces, BF16),
            jax.ShapeDtypeStruct((2 * n_layers, d_ff, 2 * width), F32),
        ),
        in_specs=[ANY] * 6 + [pl.BlockSpec(memory_space=pltpu.SMEM)],
        out_specs=(ANY, VMEM),
        scratch_shapes=[
            pltpu.VMEM((n_ex,) + pieces, BF16),
            pltpu.VMEM((n_ex,) + pieces, BF16),
            pltpu.VMEM((4, 2, 2) + pieces[1:], BF16),
            pltpu.VMEM((4, 2) + pieces[1:], BF16),
            pltpu.VMEM((4, 4, 2 * size, d_ff // 4, width), F32),
            pltpu.VMEM((size - 1, 8, 2, d_ff // 4, width), F32),
            pltpu.VMEM((2, 2) + pieces, BF16),
            pltpu.VMEM((2, 2, seq, d_ff), BF16),
            pltpu.VMEM((2 * seq, d_model), BF16),
            pltpu.VMEM((2 * seq, d_ff), BF16),
            dma((2, 4, 4, 2)),
            dma((n_ex, 2)),
            dma((4, 2)),
            dma((1,)),
            dma((2, size - 1, 8, 2)),
            dma((2, 2)),
        ],
        compiler_params=pltpu.CompilerParams(collective_id=1, has_side_effects=True, vmem_limit_bytes=66_000_000),
        name="gradient",
    )(part, dx, d_out.reshape((2, n_ex) + pieces), x.reshape((n_layers, 2, n_ex) + pieces), dh, u, clip)


def finish_kernel(examples, n_layers, d_in, up_sum, down_sum, noise_up, noise_down, clip_norm, noise_mult, up_grad, down_grad, d_in_out):
    i = pl.program_id(0)
    d_in_out[...] = d_in[...]
    noise_scale = noise_mult[0] * clip_norm[0]

    @pl.when(i < n_layers)
    def _():
        up_grad[0] = (up_sum[0].T + noise_scale * noise_up[0]) / examples

    @pl.when(i >= n_layers)
    def _():
        down_grad[0] = (down_sum[0] + noise_scale * noise_down[0]) / examples


def finish_call(examples, d_in, sums, noise_up, noise_down, clip_norm, noise_mult):
    n_layers, width, d_ff = noise_up.shape
    rows, seq, d_model = d_in.shape
    steps = 2 * n_layers

    def early(i):
        return jnp.minimum(i, n_layers - 1), 0, 0

    def late(i):
        return jnp.maximum(i - n_layers, 0), 0, 0

    def late_sum(i):
        return jnp.maximum(i, n_layers), 0, 0

    def same(i):
        return i, 0, 0

    smem = pl.BlockSpec(memory_space=pltpu.SMEM)
    block = pl.BlockSpec((rows // steps, seq, d_model), same)
    return pl.pallas_call(
        functools.partial(finish_kernel, examples, n_layers),
        grid=(steps,),
        out_shape=(
            jax.ShapeDtypeStruct((n_layers, width, d_ff), F32),
            jax.ShapeDtypeStruct((n_layers, d_ff, width), F32),
            jax.ShapeDtypeStruct(d_in.shape, BF16),
        ),
        in_specs=[
            block,
            pl.BlockSpec((1, d_ff, width), early),
            pl.BlockSpec((1, d_ff, width), late_sum),
            pl.BlockSpec((1, width, d_ff), early),
            pl.BlockSpec((1, d_ff, width), late),
            smem,
            smem,
        ],
        out_specs=(pl.BlockSpec((1, width, d_ff), early), pl.BlockSpec((1, d_ff, width), late), block),
        compiler_params=pltpu.CompilerParams(vmem_limit_bytes=66_000_000),
        name="finish",
    )(d_in, sums, sums, noise_up, noise_down, clip_norm, noise_mult)


def solution(mesh):
    dp_size = mesh.shape["dp"]

    def local_pass(x_in, u_pre, w_up, w_down, d_out, noise_up, noise_down, clip_norm, noise_mult):
        examples = d_out.shape[0] * d_out.shape[1] * dp_size
        dx, dh, part, norms = backward_call(u_pre, x_in, w_up, w_down, d_out)
        norm_vec = jnp.sum(norms, axis=2)[:, :d_out.shape[1]]
        clip_fac = jnp.minimum(1.0, clip_norm[0] / jnp.sqrt(norm_vec)).reshape(-1)
        d_in, sums = gradient_call(dp_size, part, dx, d_out, x_in, dh, u_pre, clip_fac)
        d_in = d_in.reshape((-1,) + d_out.shape[2:])
        up_grad, down_grad, d_in = finish_call(examples, d_in, sums, noise_up, noise_down, clip_norm, noise_mult)
        return up_grad, down_grad, d_in.reshape(d_out.shape)

    in_specs = (P(None, None, "dp", None, None), P(None, None, "dp", None, "tp"), P(None, None, "tp"), P(None, "tp", None), P(None, "dp", None, None), P(None, "dp", "tp"), P(None, "tp", "dp"), P(), P())
    out_specs = (P(None, "dp", "tp"), P(None, "tp", "dp"), P(None, "dp", None, None))
    return jax.shard_map(local_pass, mesh=mesh, in_specs=in_specs, out_specs=out_specs, check_vma=False)
```
